128 devices in a mesh: shard: 16 (over z, y), tp: 8 (over x, core).
Axes of the slice: x: 4, y: 4, z: 4, core: 2. Of those that a mesh axis runs over, the one named last changes fastest.
Arguments:
- train_query: bfloat16 [8192, 8192], P('shard', 'tp'), may hold values from -0.0625 to 0.0625
- low_query: bfloat16 [8192, 16], P('shard'), may hold values from -0.0625 to 0.0625
- high_query: bfloat16 [16, 8192], P(None, 'tp'), may hold values from -1.5 to 1.5
- train_key: bfloat16 [8192, 1024], P('shard', 'tp'), may hold values from -0.0625 to 0.0625
- low_key: bfloat16 [8192, 16], P('shard'), may hold values from -0.0625 to 0.0625
- high_key: bfloat16 [16, 1024], P(None, 'tp'), may hold values from -1.5 to 1.5
- train_value: bfloat16 [8192, 1024], P('shard', 'tp'), may hold values from -0.0625 to 0.0625
- low_value: bfloat16 [8192, 16], P('shard'), may hold values from -0.0625 to 0.0625
- high_value: bfloat16 [16, 1024], P(None, 'tp'), may hold values from -1.5 to 1.5
- norm_train: float32 [8192], P(('shard', 'tp')), may hold values from 0.25 to 1.75
- norm_step: float32 [8192], P(('shard', 'tp')), may hold values from -0.3 to 0.3
Outputs:
- serving_query: bfloat16 [8192, 8192], P('tp')
- serving_key: bfloat16 [1024, 8192], P('tp')
- serving_value: bfloat16 [1024, 8192], P('tp')
- serve_norm: bfloat16 [8192], replicated
The draws below stay inside these ranges and needn't reach their ends.
All inputs are finite; a program needn't handle non-finite values.
Results may differ from the reference program's by a relative error of at most 0.001.
Values may be sent and summed in bfloat16 or wider, within the bound.
A program may use at most 128 MiB of HBM per device.

```python
import jax
import jax.numpy as jnp

D_MODEL = 8192
Q_DIM = 8192
KV_DIM = 1024
RANK = 16


def shard_levels(key, extent, pieces, smallest, top_value):
    factor_of, own = 1.0, jax.random.fold_in(key, 6)
    for position, blocks in pieces:
        heights = jnp.exp(jax.random.uniform(jax.random.fold_in(own, position), (blocks,), jnp.float32, smallest / len(pieces), top_value / len(pieces)))
        factor_of = factor_of * jnp.repeat(heights, extent[position] // blocks).reshape([-1 if axis == position else 1 for axis in range(len(extent))])
    return factor_of


def normal_values(key, extent, deviation, bound, cuts=(), dtype=jnp.bfloat16):
    loudness = shard_levels(key, extent, cuts, -0.22, 0.18) if cuts else 1.0
    entries = jax.random.normal(key, extent, jnp.float32) * deviation * loudness
    return jnp.minimum(jnp.maximum(entries, -bound), bound).astype(dtype)


def setup_inputs(seed: int = 0) -> dict:
    streams_of = jax.random.split(jax.random.key(seed), 12)
    train_query = normal_values(streams_of[0], (D_MODEL, Q_DIM), D_MODEL ** -0.5, 0.0625, ((0, 16), (1, 8)))
    low_query = normal_values(streams_of[1], (D_MODEL, RANK), D_MODEL ** -0.5, 0.0625, ((0, 16),))
    high_query = normal_values(streams_of[2], (RANK, Q_DIM), RANK ** -0.5, 1.5, ((1, 8),))
    train_key = normal_values(streams_of[3], (D_MODEL, KV_DIM), D_MODEL ** -0.5, 0.0625, ((0, 16), (1, 8)))
    low_key = normal_values(streams_of[4], (D_MODEL, RANK), D_MODEL ** -0.5, 0.0625, ((0, 16),))
    high_key = normal_values(streams_of[5], (RANK, KV_DIM), RANK ** -0.5, 1.5, ((1, 8),))
    train_value = normal_values(streams_of[6], (D_MODEL, KV_DIM), D_MODEL ** -0.5, 0.0625, ((0, 16), (1, 8)))
    low_value = normal_values(streams_of[7], (D_MODEL, RANK), D_MODEL ** -0.5, 0.0625, ((0, 16),))
    high_value = normal_values(streams_of[8], (RANK, KV_DIM), RANK ** -0.5, 1.5, ((1, 8),))
    norm_train = jnp.clip(1.0 + 0.15 * jax.random.normal(streams_of[9], (D_MODEL,), jnp.float32), 0.25, 1.75)
    norm_step = jnp.clip(jax.random.uniform(streams_of[10], (D_MODEL,), jnp.float32, -0.3, 0.3) * shard_levels(streams_of[10], (D_MODEL,), ((0, 128),), -0.4, 0.0), -0.3, 0.3)
    return {"train_query": train_query, "low_query": low_query, "high_query": high_query, "train_key": train_key, "low_key": low_key, "high_key": high_key, "train_value": train_value, "low_value": low_value, "high_value": high_value, "norm_train": norm_train, "norm_step": norm_step}


mix_rate = 0.5


def reference(train_query, low_query, high_query, train_key, low_key, high_key, train_value, low_value, high_value, norm_train, norm_step):
    whole_query = train_query.astype(jnp.float32) + mix_rate * jnp.dot(low_query, high_query, preferred_element_type=jnp.float32)
    whole_key = train_key.astype(jnp.float32) + mix_rate * jnp.dot(low_key, high_key, preferred_element_type=jnp.float32)
    whole_value = train_value.astype(jnp.float32) + mix_rate * jnp.dot(low_value, high_value, preferred_element_type=jnp.float32)
    serving_query = whole_query.T.astype(jnp.bfloat16)
    serving_key = whole_key.T.astype(jnp.bfloat16)
    serving_value = whole_value.T.astype(jnp.bfloat16)
    serve_norm = (norm_train + norm_step).astype(jnp.bfloat16)
    return serving_query, serving_key, serving_value, serve_norm
```

```python
import jax
import jax.numpy as jnp
from jax import lax
from jax.experimental import pallas as pl
from jax.experimental.pallas import tpu as pltpu
from jax.sharding import PartitionSpec as P

MESH = pl.DeviceIdType.MESH
mix_rate = 0.5

ROWS, COLS, TILE = 1280, 512, 128
PART = ROWS // 4
SLOTS = 15
A, B, C, D = 0, 1, 2, 3


def schedule():
    near = (0, -1, 1, 2)
    y_up = [(0, 0, A), (0, 0, B), (-1, 0, A)]
    y_down = [(0, 0, B), (0, 0, A), (1, 0, B)]
    z_up = [(0, 0, C), (0, 0, D), (0, -1, C)]
    z_down = [(0, 0, D), (0, 0, C), (0, 1, D)]
    for far in near:
        z_up += [(far, 0, A), (far, 0, B), (far, -1, A)]
        z_down += [(far, 0, B), (far, 0, A), (far, 1, B)]
        y_up += [(0, far, C), (0, far, D), (-1, far, C)]
        y_down += [(0, far, D), (0, far, C), (1, far, D)]
    return (((1, 0), y_up), ((-1, 0), y_down), ((0, 1), z_up), ((0, -1), z_down))


LINKS = schedule()
TILES = (
    (0, ((0, 0, 128),)),
    (4, ((1, 512, 128),)),
    (5, ((2, 640, 128),)),
    (9, ((3, 1152, 128),)),
    (1, ((0, 128, 128),)),
    (3, ((1, 384, 128),)),
    (6, ((2, 768, 128),)),
    (8, ((3, 1024, 128),)),
    (2, ((0, 256, 64), (1, 320, 64))),
    (7, ((2, 896, 64), (3, 960, 64))),
)


def gather_kernel(
    tq, lq, hq, tk, lk, hk, tv, lv, hv, nt, ns,
    out, norm_out,
    t_in, l_in, h_in, nt_in, ns_in, norm_all, norm_rows,
    load_sem, send_sem, recv_sem, norm_send, norm_recv,
):
    shard, tp = lax.axis_index("shard"), lax.axis_index("tp")
    z, y = shard // 4, shard % 4
    x, core = tp // 2, tp % 2

    def at(dy, dz):
        return ((z + dz + 4) % 4) * 4 + (y + dy + 4) % 4

    def other(dx):
        return ((x + dx + 4) % 4) * 2 + core

    loads = {}

    def load(name, src, dst):
        loads[name] = pltpu.make_async_copy(src, dst, load_sem.at[len(loads)])
        loads[name].start()

    def load_tile(tile):
        if tile < 8:
            load(("t", tile), tq.at[:, pl.ds(tile * TILE, TILE)], t_in.at[tile])
        else:
            load(("t", tile), (tk, tv)[tile - 8], t_in.at[tile])

    load(("l", 0), lq, l_in.at[0])
    load(("h", 0), hq, h_in.at[:, pl.ds(0, 1024)])
    for tile, _ in TILES[:3]:
        load_tile(tile)
    load(("l", 2), lv, l_in.at[2])
    load(("h", 2), hv, h_in.at[:, pl.ds(1152, TILE)])
    for tile, _ in TILES[3:7]:
        load_tile(tile)
    load(("l", 1), lk, l_in.at[1])
    load(("h", 1), hk, h_in.at[:, pl.ds(1024, TILE)])
    for tile, _ in TILES[7:]:
        load_tile(tile)
    load("nt", nt, nt_in)
    load("ns", ns, ns_in)

    barrier = pltpu.get_barrier_semaphore()
    for (dy, dz), _ in LINKS:
        pl.semaphore_signal(barrier, inc=1, device_id={"shard": at(dy, dz)}, device_id_type=MESH)
    for peer in (x * 2 + 1 - core, other(1), other(-1)):
        pl.semaphore_signal(barrier, inc=1, device_id={"tp": peer}, device_id_type=MESH)

    def send(link, slot, rows=None):
        (ty, tz), items = LINKS[link]
        dy, dz, part = items[slot]
        row, count = rows if rows is not None else (part * PART, PART)
        piece = out.at[at(dy, dz), pl.ds(row, count)]
        return pltpu.make_async_remote_copy(
            src_ref=piece, dst_ref=piece, send_sem=send_sem.at[link, slot], recv_sem=recv_sem.at[link, slot],
            device_id={"shard": at(ty, tz)}, device_id_type=MESH,
        )

    def arrival(link, slot):
        (ty, tz), items = LINKS[link]
        dy, dz, part = items[slot]
        piece = out.at[at(dy - ty, dz - tz), pl.ds(part * PART, PART)]
        return pltpu.make_async_remote_copy(
            src_ref=piece, dst_ref=piece, send_sem=send_sem.at[link, slot], recv_sem=recv_sem.at[link, slot],
            device_id={"shard": at(ty, tz)}, device_id_type=MESH,
        )

    def merge(tile):
        loads[("t", tile)].wait()
        which = max(tile - 7, 0)
        for name in (("l", which), ("h", which)):
            if name in loads:
                loads.pop(name).wait()
        product = lax.dot_general(
            h_in[:, tile * TILE:(tile + 1) * TILE], l_in[which], (((0,), (0,)), ((), ())),
            preferred_element_type=jnp.float32,
        )
        whole = t_in[tile].astype(jnp.float32).T + mix_rate * product
        out[shard, tile * TILE:(tile + 1) * TILE, :] = whole.astype(jnp.bfloat16)

    waiting = ()
    for place, (tile, pieces) in enumerate(TILES):
        merge(tile)
        if place == 1:
            pl.semaphore_wait(barrier, 7)
        for link, row, count in waiting:
            send(link, 0, (row, count)).start()
        waiting = pieces
    for link, row, count in waiting:
        send(link, 0, (row, count)).start()
    for link in range(4):
        send(link, 1).start()

    loads["nt"].wait()
    loads["ns"].wait()
    gain = nt_in[...] + ns_in[...]
    both = jnp.concatenate([gain, gain], axis=1)
    half = lax.broadcasted_iota(jnp.int32, (1, 128), 1) // 64
    norm_all[shard, tp] = jnp.where(half == core, both, 0.0)

    def norm_copy(step, piece, peer):
        return pltpu.make_async_remote_copy(
            src_ref=piece, dst_ref=piece, send_sem=norm_send.at[step], recv_sem=norm_recv.at[step],
            device_id=peer, device_id_type=MESH,
        )

    def pair(dx):
        return norm_all.at[shard, pl.ds(((x + dx + 4) % 4) * 2, 2)]

    def row_of(dy):
        return norm_all.at[at(dy, 0)]

    def plane_of(dz):
        return norm_all.at[pl.ds(((z + dz + 4) % 4) * 4, 4)]

    own = norm_all.at[shard, tp]
    twin = norm_all.at[shard, x * 2 + 1 - core]
    norm_steps = (
        ((0, own, {"tp": x * 2 + 1 - core}, twin),),
        ((1, pair(0), {"tp": other(1)}, pair(-1)), (2, pair(0), {"tp": other(-1)}, pair(1))),
        ((3, pair(-1), {"tp": other(1)}, pair(2)),),
        ((4, row_of(0), {"shard": at(1, 0)}, row_of(-1)), (5, row_of(0), {"shard": at(-1, 0)}, row_of(1))),
        ((6, row_of(-1), {"shard": at(1, 0)}, row_of(2)),),
        ((7, plane_of(0), {"shard": at(0, 1)}, plane_of(-1)), (8, plane_of(0), {"shard": at(0, -1)}, plane_of(1))),
        ((9, plane_of(-1), {"shard": at(0, 1)}, plane_of(2)),),
    )

    def norm_start(step):
        for sem, sent, peer, _ in norm_steps[step]:
            norm_copy(sem, sent, peer).start()

    def norm_wait(step):
        for sem, sent, peer, arrived in norm_steps[step]:
            norm_copy(sem, sent, peer).wait_send()
            norm_copy(sem, arrived, peer).wait_recv()

    norm_start(0)
    for slot in range(SLOTS):
        for link in range(4):
            arrival(link, slot).wait_recv()
        if slot < len(norm_steps):
            norm_wait(slot)
        if slot + 1 < len(norm_steps):
            norm_start(slot + 1)
        if slot + 2 < SLOTS:
            for link in range(4):
                send(link, slot + 2).start()
        if slot == len(norm_steps):
            for row in range(64):
                first = norm_all[row // 4, (row % 4) * 2]
                second = norm_all[row // 4, (row % 4) * 2 + 1]
                norm_rows[row:row + 1, :] = first + second
            norm_out[...] = norm_rows[...].astype(jnp.bfloat16)
    for slot in range(SLOTS):
        for link in range(4):
            (_, _), items = LINKS[link]
            send(link, slot).wait_send()


def write_kernel(block, norm, q, k, v, n, sem):
    copies = []

    def copy(src, dst):
        copies.append(pltpu.make_async_copy(src, dst, sem.at[len(copies)]))
        copies[-1].start()

    for s in range(16):
        columns = pl.ds(s * COLS, COLS)
        copy(block.at[s, pl.ds(0, 1024)], q.at[:, columns])
        copy(block.at[s, pl.ds(1024, 128)], k.at[:, columns])
        copy(block.at[s, pl.ds(1152, 128)], v.at[:, columns])
    copy(norm, n)
    for c in copies:
        c.wait()


def per_device(tq, lq, hq, tk, lk, hk, tv, lv, hv, nt, ns):
    hbm = pl.BlockSpec(memory_space=pltpu.HBM)
    vmem = pl.BlockSpec(memory_space=pltpu.VMEM)
    bf16, f32 = jnp.bfloat16, jnp.float32
    block, norm = pl.pallas_call(
        gather_kernel,
        out_shape=(pltpu.VMEM((16, ROWS, COLS), bf16), pltpu.VMEM((64, 128), bf16)),
        in_specs=[hbm] * 11,
        out_specs=(vmem, vmem),
        scratch_shapes=[
            pltpu.VMEM((10, COLS, TILE), bf16),
            pltpu.VMEM((3, 16, COLS), bf16),
            pltpu.VMEM((16, ROWS), bf16),
            pltpu.VMEM((1, 64), f32),
            pltpu.VMEM((1, 64), f32),
            pltpu.VMEM((16, 8, 1, 128), f32),
            pltpu.VMEM((64, 128), f32),
            pltpu.SemaphoreType.DMA((18,)),
            pltpu.SemaphoreType.DMA((4, SLOTS)),
            pltpu.SemaphoreType.DMA((4, SLOTS)),
            pltpu.SemaphoreType.DMA((10,)),
            pltpu.SemaphoreType.DMA((10,)),
        ],
        compiler_params=pltpu.CompilerParams(
            collective_id=0, has_side_effects=True, vmem_limit_bytes=12 * 1024 * 1024
        ),
        name="gather",
    )(*(
        pltpu.with_memory_space_constraint(a, pltpu.HBM)
        for a in (tq, lq.T, hq, tk, lk.T, hk, tv, lv.T, hv, nt.reshape(1, 64), ns.reshape(1, 64))
    ))
    q, k, v, n = pl.pallas_call(
        write_kernel,
        out_shape=(
            jax.ShapeDtypeStruct((1024, 8192), bf16),
            jax.ShapeDtypeStruct((128, 8192), bf16),
            jax.ShapeDtypeStruct((128, 8192), bf16),
            jax.ShapeDtypeStruct((64, 128), bf16),
        ),
        in_specs=[vmem, vmem],
        out_specs=(hbm,) * 4,
        scratch_shapes=[pltpu.SemaphoreType.DMA((49,))],
        compiler_params=pltpu.CompilerParams(vmem_limit_bytes=12 * 1024 * 1024),
        name="write",
    )(block, norm)
    return q, k, v, n.reshape(8192)


def solution(mesh):
    in_specs = (
        P("shard", "tp"), P("shard", None), P(None, "tp"),
        P("shard", "tp"), P("shard", None), P(None, "tp"),
        P("shard", "tp"), P("shard", None), P(None, "tp"),
        P(("shard", "tp")), P(("shard", "tp")),
    )
    out_specs = (P("tp", None), P("tp", None), P("tp", None), P())
    return jax.shard_map(per_device, mesh=mesh, in_specs=in_specs, out_specs=out_specs, check_vma=False)
```

```python
import jax
import jax.numpy as jnp
from jax import lax
from jax.experimental import pallas as pl
from jax.experimental.pallas import tpu as pltpu
from jax.sharding import PartitionSpec as P

MESH = pl.DeviceIdType.MESH
mix_rate = 0.5

ROWS, COLS, TILE = 1280, 512, 128
PART = ROWS // 4
SLOTS = 15
A, B, C, D = 0, 1, 2, 3


def schedule():
    def order(first, second, own_first, own_second, step, place):
        side = lambda far: place(0, far)
        return [
            side(0) + (first,), side(0) + (second,), side(0) + (own_first,), side(0) + (own_second,),
            place(-step, 0) + (first,),
            side(-1) + (own_first,), side(-1) + (own_second,),
            place(-step, 0) + (own_first,),
            side(1) + (own_first,), side(1) + (own_second,),
            side(2) + (own_first,), side(2) + (own_second,),
            place(-step, -1) + (own_first,), place(-step, 1) + (own_first,), place(-step, 2) + (own_first,),
        ]

    along_y = lambda along, across: (along, across)
    along_z = lambda along, across: (across, along)
    return (
        ((1, 0), order(A, B, C, D, 1, along_y)),
        ((-1, 0), order(B, A, D, C, -1, along_y)),
        ((0, 1), order(C, D, A, B, 1, along_z)),
        ((0, -1), order(D, C, B, A, -1, along_z)),
    )


AHEAD = 4
LINKS = schedule()
TILES = (
    (0, ((0, 0, 0, 128), (1, 1, 0, 128))),
    (5, ((2, 0, 640, 128), (3, 1, 640, 128))),
    (4, ((1, 0, 512, 128),)),
    (9, ((3, 0, 1152, 128),)),
    (1, ((0, 0, 128, 128),)),
    (6, ((2, 0, 768, 128),)),
    (3, ((1, 0, 384, 128),)),
    (8, ((3, 0, 1024, 128),)),
    (2, ((0, 0, 256, 64), (1, 0, 320, 64), (1, 1, 128, 192))),
    (7, ((2, 0, 896, 64), (3, 0, 960, 64), (3, 1, 768, 192))),
)


def gather_kernel(
    tq, lq, hq, tk, lk, hk, tv, lv, hv, nt, ns,
    out, norm_out,
    t_in, l_in, h_in, nt_in, ns_in, norm_all, norm_rows,
    load_sem, send_sem, recv_sem, norm_send, norm_recv,
):
    shard, tp = lax.axis_index("shard"), lax.axis_index("tp")
    z, y = shard // 4, shard % 4
    x, core = tp // 2, tp % 2

    def at(dy, dz):
        return ((z + dz + 4) % 4) * 4 + (y + dy + 4) % 4

    def other(dx):
        return ((x + dx + 4) % 4) * 2 + core

    loads = {}

    def load(name, src, dst):
        loads[name] = pltpu.make_async_copy(src, dst, load_sem.at[len(loads)])
        loads[name].start()

    def load_tile(tile):
        if tile < 8:
            load(("t", tile), tq.at[:, pl.ds(tile * TILE, TILE)], t_in.at[tile])
        else:
            load(("t", tile), (tk, tv)[tile - 8], t_in.at[tile])

    load(("l", 0), lq, l_in.at[0])
    load(("h", 0), hq, h_in.at[:, pl.ds(0, 1024)])
    for tile, _ in TILES[:3]:
        load_tile(tile)
    load(("l", 2), lv, l_in.at[2])
    load(("h", 2), hv, h_in.at[:, pl.ds(1152, TILE)])
    for tile, _ in TILES[3:7]:
        load_tile(tile)
    load(("l", 1), lk, l_in.at[1])
    load(("h", 1), hk, h_in.at[:, pl.ds(1024, TILE)])
    for tile, _ in TILES[7:]:
        load_tile(tile)
    load("nt", nt, nt_in)
    load("ns", ns, ns_in)

    barrier = pltpu.get_barrier_semaphore()
    for (dy, dz), _ in LINKS:
        pl.semaphore_signal(barrier, inc=1, device_id={"shard": at(dy, dz)}, device_id_type=MESH)
    for peer in (x * 2 + 1 - core, other(1), other(-1)):
        pl.semaphore_signal(barrier, inc=1, device_id={"tp": peer}, device_id_type=MESH)

    def send(link, slot, rows=None):
        (ty, tz), items = LINKS[link]
        dy, dz, part = items[slot]
        row, count = rows if rows is not None else (part * PART, PART)
        piece = out.at[at(dy, dz), pl.ds(row, count)]
        return pltpu.make_async_remote_copy(
            src_ref=piece, dst_ref=piece, send_sem=send_sem.at[link, slot], recv_sem=recv_sem.at[link, slot],
            device_id={"shard": at(ty, tz)}, device_id_type=MESH,
        )

    def arrival(link, slot):
        (ty, tz), items = LINKS[link]
        dy, dz, part = items[slot]
        piece = out.at[at(dy - ty, dz - tz), pl.ds(part * PART, PART)]
        return pltpu.make_async_remote_copy(
            src_ref=piece, dst_ref=piece, send_sem=send_sem.at[link, slot], recv_sem=recv_sem.at[link, slot],
            device_id={"shard": at(ty, tz)}, device_id_type=MESH,
        )

    def merge(tile):
        loads[("t", tile)].wait()
        which = max(tile - 7, 0)
        for name in (("l", which), ("h", which)):
            if name in loads:
                loads.pop(name).wait()
        product = lax.dot_general(
            h_in[:, tile * TILE:(tile + 1) * TILE], l_in[which], (((0,), (0,)), ((), ())),
            preferred_element_type=jnp.float32,
        )
        whole = t_in[tile].astype(jnp.float32).T + mix_rate * product
        out[shard, tile * TILE:(tile + 1) * TILE, :] = whole.astype(jnp.bfloat16)

    waiting = ()
    for place, (tile, pieces) in enumerate(TILES):
        merge(tile)
        if place == 1:
            pl.semaphore_wait(barrier, 7)
        for link, slot, row, count in waiting:
            send(link, slot, (row, count)).start()
        waiting = pieces
    for link, slot, row, count in waiting:
        send(link, slot, (row, count)).start()
    for link in (0, 2):
        send(link, 1).start()
    for slot in range(2, AHEAD):
        for link in range(4):
            send(link, slot).start()

    loads["nt"].wait()
    loads["ns"].wait()
    gain = nt_in[...] + ns_in[...]
    both = jnp.concatenate([gain, gain], axis=1)
    half = lax.broadcasted_iota(jnp.int32, (1, 128), 1) // 64
    norm_all[shard, tp] = jnp.where(half == core, both, 0.0)

    def norm_copy(step, piece, peer):
        return pltpu.make_async_remote_copy(
            src_ref=piece, dst_ref=piece, send_sem=norm_send.at[step], recv_sem=norm_recv.at[step],
            device_id=peer, device_id_type=MESH,
        )

    def pair(dx):
        return norm_all.at[shard, pl.ds(((x + dx + 4) % 4) * 2, 2)]

    def row_of(dy):
        return norm_all.at[at(dy, 0)]

    def plane_of(dz):
        return norm_all.at[pl.ds(((z + dz + 4) % 4) * 4, 4)]

    own = norm_all.at[shard, tp]
    twin = norm_all.at[shard, x * 2 + 1 - core]
    norm_steps = (
        ((0, own, {"tp": x * 2 + 1 - core}, twin),),
        ((1, pair(0), {"tp": other(1)}, pair(-1)), (2, pair(0), {"tp": other(-1)}, pair(1))),
        ((3, pair(-1), {"tp": other(1)}, pair(2)),),
        ((4, row_of(0), {"shard": at(1, 0)}, row_of(-1)), (5, row_of(0), {"shard": at(-1, 0)}, row_of(1))),
        ((6, row_of(-1), {"shard": at(1, 0)}, row_of(2)),),
        ((7, plane_of(0), {"shard": at(0, 1)}, plane_of(-1)), (8, plane_of(0), {"shard": at(0, -1)}, plane_of(1))),
        ((9, plane_of(-1), {"shard": at(0, 1)}, plane_of(2)),),
    )

    def norm_start(step):
        for sem, sent, peer, _ in norm_steps[step]:
            norm_copy(sem, sent, peer).start()

    def norm_wait(step):
        for sem, sent, peer, arrived in norm_steps[step]:
            norm_copy(sem, sent, peer).wait_send()
            norm_copy(sem, arrived, peer).wait_recv()

    norm_start(0)
    for slot in range(SLOTS):
        for link in range(4):
            arrival(link, slot).wait_recv()
        if slot < len(norm_steps):
            norm_wait(slot)
        if slot + 1 < len(norm_steps):
            norm_start(slot + 1)
        if slot + AHEAD < SLOTS:
            for link in range(4):
                send(link, slot + AHEAD).start()
        if slot == len(norm_steps):
            for row in range(64):
                first = norm_all[row // 4, (row % 4) * 2]
                second = norm_all[row // 4, (row % 4) * 2 + 1]
                norm_rows[row:row + 1, :] = first + second
            norm_out[...] = norm_rows[...].astype(jnp.bfloat16)
    for slot in range(SLOTS):
        for link in range(4):
            (_, _), items = LINKS[link]
            send(link, slot).wait_send()


def write_kernel(block, norm, q, k, v, n, sem):
    copies = []

    def copy(src, dst):
        copies.append(pltpu.make_async_copy(src, dst, sem.at[len(copies)]))
        copies[-1].start()

    for s in range(16):
        columns = pl.ds(s * COLS, COLS)
        copy(block.at[s, pl.ds(0, 1024)], q.at[:, columns])
        copy(block.at[s, pl.ds(1024, 128)], k.at[:, columns])
        copy(block.at[s, pl.ds(1152, 128)], v.at[:, columns])
    copy(norm, n)
    for c in copies:
        c.wait()


def per_device(tq, lq, hq, tk, lk, hk, tv, lv, hv, nt, ns):
    hbm = pl.BlockSpec(memory_space=pltpu.HBM)
    vmem = pl.BlockSpec(memory_space=pltpu.VMEM)
    bf16, f32 = jnp.bfloat16, jnp.float32
    block, norm = pl.pallas_call(
        gather_kernel,
        out_shape=(pltpu.VMEM((16, ROWS, COLS), bf16), pltpu.VMEM((64, 128), bf16)),
        in_specs=[hbm] * 11,
        out_specs=(vmem, vmem),
        scratch_shapes=[
            pltpu.VMEM((10, COLS, TILE), bf16),
            pltpu.VMEM((3, 16, COLS), bf16),
            pltpu.VMEM((16, ROWS), bf16),
            pltpu.VMEM((1, 64), f32),
            pltpu.VMEM((1, 64), f32),
            pltpu.VMEM((16, 8, 1, 128), f32),
            pltpu.VMEM((64, 128), f32),
            pltpu.SemaphoreType.DMA((18,)),
            pltpu.SemaphoreType.DMA((4, SLOTS)),
            pltpu.SemaphoreType.DMA((4, SLOTS)),
            pltpu.SemaphoreType.DMA((10,)),
            pltpu.SemaphoreType.DMA((10,)),
        ],
        compiler_params=pltpu.CompilerParams(
            collective_id=0, has_side_effects=True, vmem_limit_bytes=12 * 1024 * 1024
        ),
        name="gather",
    )(*(
        pltpu.with_memory_space_constraint(a, pltpu.HBM)
        for a in (tq, lq.T, hq, tk, lk.T, hk, tv, lv.T, hv, nt.reshape(1, 64), ns.reshape(1, 64))
    ))
    q, k, v, n = pl.pallas_call(
        write_kernel,
        out_shape=(
            jax.ShapeDtypeStruct((1024, 8192), bf16),
            jax.ShapeDtypeStruct((128, 8192), bf16),
            jax.ShapeDtypeStruct((128, 8192), bf16),
            jax.ShapeDtypeStruct((64, 128), bf16),
        ),
        in_specs=[vmem, vmem],
        out_specs=(hbm,) * 4,
        scratch_shapes=[pltpu.SemaphoreType.DMA((49,))],
        compiler_params=pltpu.CompilerParams(vmem_limit_bytes=12 * 1024 * 1024),
        name="write",
    )(block, norm)
    return q, k, v, n.reshape(8192)


def solution(mesh):
    in_specs = (
        P("shard", "tp"), P("shard", None), P(None, "tp"),
        P("shard", "tp"), P("shard", None), P(None, "tp"),
        P("shard", "tp"), P("shard", None), P(None, "tp"),
        P(("shard", "tp")), P(("shard", "tp")),
    )
    out_specs = (P("tp", None), P("tp", None), P("tp", None), P())
    return jax.shard_map(per_device, mesh=mesh, in_specs=in_specs, out_specs=out_specs, check_vma=False)
```

```python
import jax
import jax.numpy as jnp
from jax import lax
from jax.experimental import pallas as pl
from jax.experimental.pallas import tpu as pltpu
from jax.sharding import PartitionSpec as P

MESH = pl.DeviceIdType.MESH
mix_rate = 0.5

ROWS, COLS, TILE = 1280, 512, 128
PART = ROWS // 4
SLOTS = 15
A, B, C, D = 0, 1, 2, 3


def schedule():
    def order(first, second, own_first, own_second, step, place):
        side = lambda far: place(0, far)
        return [
            side(0) + (first,), side(0) + (second,), side(0) + (own_first,), side(0) + (own_second,),
            place(-step, 0) + (first,),
            side(-1) + (own_first,), side(-1) + (own_second,),
            place(-step, 0) + (own_first,),
            side(1) + (own_first,), side(1) + (own_second,),
            side(2) + (own_first,), side(2) + (own_second,),
            place(-step, -1) + (own_first,), place(-step, 1) + (own_first,), place(-step, 2) + (own_first,),
        ]

    along_y = lambda along, across: (along, across)
    along_z = lambda along, across: (across, along)
    return (
        ((1, 0), order(A, B, C, D, 1, along_y)),
        ((-1, 0), order(B, A, D, C, -1, along_y)),
        ((0, 1), order(C, D, A, B, 1, along_z)),
        ((0, -1), order(D, C, B, A, -1, along_z)),
    )


AHEAD = 4
BREAK = (10, 13)
LATE = SLOTS - BREAK[0]
LINKS = schedule()
ARRIVALS = [
    [(((dy - ty + 1) % 4) - 1, ((dz - tz + 1) % 4) - 1, part) for dy, dz, part in items] for (ty, tz), items in LINKS
]
PLACE = {ARRIVALS[link][slot]: (link, slot) for link in range(4) for slot in range(SLOTS)}
TILES = (
    (0, ((0, 0, 0, 128), (1, 1, 0, 128))),
    (5, ((2, 0, 640, 128), (3, 1, 640, 128))),
    (4, ((1, 0, 512, 128),)),
    (9, ((3, 0, 1152, 128),)),
    (1, ((0, 0, 128, 128),)),
    (6, ((2, 0, 768, 128),)),
    (3, ((1, 0, 384, 128),)),
    (8, ((3, 0, 1024, 128),)),
    (2, ((0, 0, 256, 64), (1, 0, 320, 64), (1, 1, 128, 192))),
    (7, ((2, 0, 896, 64), (3, 0, 960, 64), (3, 1, 768, 192))),
)


def position():
    shard, core = lax.axis_index("shard"), lax.axis_index("tp") % 2
    z, y = shard // 4, shard % 4

    def at(dy, dz):
        return ((z + dz + 4) % 4) * 4 + (y + dy + 4) % 4

    return shard, core, at


def gather_kernel(
    tq, lq, hq, tk, lk, hk, tv, lv, hv, nt, ns,
    out, norm_out,
    t_in, l_in, h_in, nt_in, ns_in, norm_all, norm_rows,
    load_sem, send_sem, recv_sem, norm_send, norm_recv,
):
    shard, core, at = position()
    tp = lax.axis_index("tp")
    z, x = shard // 4, tp // 2

    def other(dx):
        return ((x + dx + 4) % 4) * 2 + core

    loads = {}

    def load(name, src, dst):
        loads[name] = pltpu.make_async_copy(src, dst, load_sem.at[len(loads)])
        loads[name].start()

    def load_tile(tile):
        if tile < 8:
            load(("t", tile), tq.at[:, pl.ds(tile * TILE, TILE)], t_in.at[tile])
        else:
            load(("t", tile), (tk, tv)[tile - 8], t_in.at[tile])

    load(("l", 0), lq, l_in.at[0])
    load(("h", 0), hq, h_in.at[:, pl.ds(0, 1024)])
    for tile, _ in TILES[:3]:
        load_tile(tile)
    load(("l", 2), lv, l_in.at[2])
    load(("h", 2), hv, h_in.at[:, pl.ds(1152, TILE)])
    for tile, _ in TILES[3:7]:
        load_tile(tile)
    load(("l", 1), lk, l_in.at[1])
    load(("h", 1), hk, h_in.at[:, pl.ds(1024, TILE)])
    for tile, _ in TILES[7:]:
        load_tile(tile)
    load("nt", nt, nt_in)
    load("ns", ns, ns_in)

    barrier = pltpu.get_barrier_semaphore()
    for (dy, dz), _ in LINKS:
        pl.semaphore_signal(barrier, inc=1, device_id={"shard": at(dy, dz)}, device_id_type=MESH)
    for peer in (x * 2 + 1 - core, other(1), other(-1)):
        pl.semaphore_signal(barrier, inc=1, device_id={"tp": peer}, device_id_type=MESH)

    def send(link, slot, rows=None):
        (ty, tz), items = LINKS[link]
        dy, dz, part = items[slot]
        row, count = rows if rows is not None else (part * PART, PART)
        piece = out.at[at(dy, dz), pl.ds(row, count)]
        return pltpu.make_async_remote_copy(
            src_ref=piece, dst_ref=piece, send_sem=send_sem.at[link, slot], recv_sem=recv_sem.at[link, slot],
            device_id={"shard": at(ty, tz)}, device_id_type=MESH,
        )

    def arrival(link, slot):
        (ty, tz), items = LINKS[link]
        dy, dz, part = items[slot]
        piece = out.at[at(dy - ty, dz - tz), pl.ds(part * PART, PART)]
        return pltpu.make_async_remote_copy(
            src_ref=piece, dst_ref=piece, send_sem=send_sem.at[link, slot], recv_sem=recv_sem.at[link, slot],
            device_id={"shard": at(ty, tz)}, device_id_type=MESH,
        )

    def merge(tile):
        loads[("t", tile)].wait()
        which = max(tile - 7, 0)
        for name in (("l", which), ("h", which)):
            if name in loads:
                loads.pop(name).wait()
        product = lax.dot_general(
            h_in[:, tile * TILE:(tile + 1) * TILE], l_in[which], (((0,), (0,)), ((), ())),
            preferred_element_type=jnp.float32,
        )
        whole = t_in[tile].astype(jnp.float32).T + mix_rate * product
        out[shard, tile * TILE:(tile + 1) * TILE, :] = whole.astype(jnp.bfloat16)

    waiting = ()
    for place, (tile, pieces) in enumerate(TILES):
        merge(tile)
        if place == 1:
            pl.semaphore_wait(barrier, 7)
        for link, slot, row, count in waiting:
            send(link, slot, (row, count)).start()
        waiting = pieces
    for link, slot, row, count in waiting:
        send(link, slot, (row, count)).start()
    for link in (0, 2):
        send(link, 1).start()
    for slot in range(2, AHEAD):
        for link in range(4):
            send(link, slot).start()

    loads["nt"].wait()
    loads["ns"].wait()
    gain = nt_in[...] + ns_in[...]
    both = jnp.concatenate([gain, gain], axis=1)
    half = lax.broadcasted_iota(jnp.int32, (1, 128), 1) // 64
    norm_all[shard, tp] = jnp.where(half == core, both, 0.0)

    def norm_copy(step, piece, peer):
        return pltpu.make_async_remote_copy(
            src_ref=piece, dst_ref=piece, send_sem=norm_send.at[step], recv_sem=norm_recv.at[step],
            device_id=peer, device_id_type=MESH,
        )

    def pair(dx):
        return norm_all.at[shard, pl.ds(((x + dx + 4) % 4) * 2, 2)]

    def row_of(dy):
        return norm_all.at[at(dy, 0)]

    def plane_of(dz):
        return norm_all.at[pl.ds(((z + dz + 4) % 4) * 4, 4)]

    own = norm_all.at[shard, tp]
    twin = norm_all.at[shard, x * 2 + 1 - core]
    norm_steps = (
        ((0, own, {"tp": x * 2 + 1 - core}, twin),),
        ((1, pair(0), {"tp": other(1)}, pair(-1)), (2, pair(0), {"tp": other(-1)}, pair(1))),
        ((3, pair(-1), {"tp": other(1)}, pair(2)),),
        ((4, row_of(0), {"shard": at(1, 0)}, row_of(-1)), (5, row_of(0), {"shard": at(-1, 0)}, row_of(1))),
        ((6, row_of(-1), {"shard": at(1, 0)}, row_of(2)),),
        ((7, plane_of(0), {"shard": at(0, 1)}, plane_of(-1)), (8, plane_of(0), {"shard": at(0, -1)}, plane_of(1))),
        ((9, plane_of(-1), {"shard": at(0, 1)}, plane_of(2)),),
    )

    def norm_start(step):
        for sem, sent, peer, _ in norm_steps[step]:
            norm_copy(sem, sent, peer).start()

    def norm_wait(step):
        for sem, sent, peer, arrived in norm_steps[step]:
            norm_copy(sem, sent, peer).wait_send()
            norm_copy(sem, arrived, peer).wait_recv()

    def launch(slot):
        for link in range(4):
            send(link, slot).start()

    def receive(slot):
        for link in range(4):
            arrival(link, slot).wait_recv()

    def sent(slots):
        for slot in slots:
            for link in range(4):
                send(link, slot).wait_send()

    norm_start(0)
    first, last = BREAK
    for slot in range(first):
        receive(slot)
        if slot < len(norm_steps):
            norm_wait(slot)
        if slot + 1 < len(norm_steps):
            norm_start(slot + 1)
        if slot + AHEAD < first:
            launch(slot + AHEAD)
        elif slot + AHEAD < last:
            pl.when(core == 1)(lambda: launch(slot + AHEAD))
        if slot == len(norm_steps):
            for row in range(64):
                even = norm_all[row // 4, (row % 4) * 2]
                odd = norm_all[row // 4, (row % 4) * 2 + 1]
                norm_rows[row:row + 1, :] = even + odd
            norm_out[...] = norm_rows[...].astype(jnp.bfloat16)

    @pl.when(core == 1)
    def _():
        for slot in range(first, last):
            receive(slot)
            if slot + AHEAD < last:
                launch(slot + AHEAD)
        sent(range(first, last))

    sent(range(first))


def rest_kernel(block, norm, rest, send_sem, recv_sem):
    _, core, at = position()
    barrier = pltpu.get_barrier_semaphore()
    for (dy, dz), _ in LINKS:
        pl.semaphore_signal(barrier, inc=1, device_id={"shard": at(dy, dz)}, device_id_type=MESH)
    pl.semaphore_wait(barrier, 4)

    def run(first):
        def copy(link, slot):
            (ty, tz), items = LINKS[link]
            dy, dz, part = items[slot]
            from_link, from_slot = PLACE.get(((dy + 1) % 4 - 1, (dz + 1) % 4 - 1, part), (0, -1))
            if from_slot < first:
                piece = block.at[at(dy, dz), pl.ds(part * PART, PART)]
            else:
                piece = rest.at[from_link, from_slot - first]
            return pltpu.make_async_remote_copy(
                src_ref=piece, dst_ref=rest.at[link, slot - first],
                send_sem=send_sem.at[link, slot - first], recv_sem=recv_sem.at[link, slot - first],
                device_id={"shard": at(ty, tz)}, device_id_type=MESH,
            )

        for slot in range(first, min(first + AHEAD, SLOTS)):
            for link in range(4):
                copy(link, slot).start()
        for slot in range(first, SLOTS):
            for link in range(4):
                copy(link, slot).wait_recv()
            if slot + AHEAD < SLOTS:
                for link in range(4):
                    copy(link, slot + AHEAD).start()
        for slot in range(first, SLOTS):
            for link in range(4):
                copy(link, slot).wait_send()

    for which in range(2):
        pl.when(core == which)(lambda: run(BREAK[which]))


def write_part(copies, sem, src, owner, part, q, k, v):
    columns = pl.ds(pl.multiple_of(owner * COLS, COLS), COLS)
    row, count = part * PART, min(PART, 1024 - part * PART)
    pieces = [(0, count, q.at[pl.ds(row, count), columns])]
    if part == D:
        pieces += [(64, 128, k.at[:, columns]), (192, 128, v.at[:, columns])]
    for start, rows, dst in pieces:
        copies.append(pltpu.make_async_copy(src.at[pl.ds(start, rows)], dst, sem.at[len(copies)]))
        copies[-1].start()


def write_kernel(block, norm, q, k, v, n, sem):
    shard, core, at = position()

    def run(first):
        copies = []
        for part in range(4):
            for far in range(16):
                dy, dz = far % 4 - 1, far // 4 - 1
                if PLACE.get((dy, dz, part), (0, -1))[1] < first:
                    src = block.at[at(dy, dz), pl.ds(part * PART, PART)]
                    write_part(copies, sem, src, at(dy, dz), part, q, k, v)
        copies.append(pltpu.make_async_copy(norm, n, sem.at[len(copies)]))
        copies[-1].start()
        for c in copies:
            c.wait()

    for which in range(2):
        pl.when(core == which)(lambda: run(BREAK[which]))


def write_rest_kernel(rest, q_in, k_in, v_in, q, k, v, sem):
    _, core, at = position()

    def run(first):
        copies = []
        for (dy, dz, part), (link, slot) in PLACE.items():
            if slot >= first:
                write_part(copies, sem, rest.at[link, slot - first], at(dy, dz), part, q, k, v)
        for c in copies:
            c.wait()

    for which in range(2):
        pl.when(core == which)(lambda: run(BREAK[which]))


def per_device(tq, lq, hq, tk, lk, hk, tv, lv, hv, nt, ns):
    hbm = pl.BlockSpec(memory_space=pltpu.HBM)
    vmem = pl.BlockSpec(memory_space=pltpu.VMEM)
    bf16, f32 = jnp.bfloat16, jnp.float32
    block, norm = pl.pallas_call(
        gather_kernel,
        out_shape=(pltpu.VMEM((16, ROWS, COLS), bf16), pltpu.VMEM((64, 128), bf16)),
        in_specs=[hbm] * 11,
        out_specs=(vmem, vmem),
        scratch_shapes=[
            pltpu.VMEM((10, COLS, TILE), bf16),
            pltpu.VMEM((3, 16, COLS), bf16),
            pltpu.VMEM((16, ROWS), bf16),
            pltpu.VMEM((1, 64), f32),
            pltpu.VMEM((1, 64), f32),
            pltpu.VMEM((16, 8, 1, 128), f32),
            pltpu.VMEM((64, 128), f32),
            pltpu.SemaphoreType.DMA((18,)),
            pltpu.SemaphoreType.DMA((4, SLOTS)),
            pltpu.SemaphoreType.DMA((4, SLOTS)),
            pltpu.SemaphoreType.DMA((10,)),
            pltpu.SemaphoreType.DMA((10,)),
        ],
        compiler_params=pltpu.CompilerParams(
            collective_id=0, has_side_effects=True, vmem_limit_bytes=12 * 1024 * 1024
        ),
        name="gather",
    )(*(
        pltpu.with_memory_space_constraint(a, pltpu.HBM)
        for a in (tq, lq.T, hq, tk, lk.T, hk, tv, lv.T, hv, nt.reshape(1, 64), ns.reshape(1, 64))
    ))
    results = (
        jax.ShapeDtypeStruct((1024, 8192), bf16),
        jax.ShapeDtypeStruct((128, 8192), bf16),
        jax.ShapeDtypeStruct((128, 8192), bf16),
    )
    q, k, v, n = pl.pallas_call(
        write_kernel,
        out_shape=results + (jax.ShapeDtypeStruct((64, 128), bf16),),
        in_specs=[vmem, vmem],
        out_specs=(hbm,) * 4,
        scratch_shapes=[pltpu.SemaphoreType.DMA((100,))],
        compiler_params=pltpu.CompilerParams(vmem_limit_bytes=4 * 1024 * 1024),
        name="write",
    )(block, norm)
    rest = pl.pallas_call(
        rest_kernel,
        out_shape=pltpu.VMEM((4, LATE, PART, COLS), bf16),
        in_specs=[vmem, hbm],
        out_specs=vmem,
        scratch_shapes=[pltpu.SemaphoreType.DMA((4, LATE)), pltpu.SemaphoreType.DMA((4, LATE))],
        compiler_params=pltpu.CompilerParams(
            collective_id=1, has_side_effects=True, vmem_limit_bytes=4 * 1024 * 1024
        ),
        name="rest",
    )(block, pltpu.with_memory_space_constraint(n, pltpu.HBM))
    q, k, v = pl.pallas_call(
        write_rest_kernel,
        out_shape=results,
        in_specs=[vmem] + [hbm] * 3,
        out_specs=(hbm,) * 3,
        input_output_aliases={1: 0, 2: 1, 3: 2},
        scratch_shapes=[pltpu.SemaphoreType.DMA((100,))],
        compiler_params=pltpu.CompilerParams(vmem_limit_bytes=4 * 1024 * 1024),
        name="write_rest",
    )(rest, *(pltpu.with_memory_space_constraint(a, pltpu.HBM) for a in (q, k, v)))
    return q, k, v, n.reshape(8192)


def solution(mesh):
    in_specs = (
        P("shard", "tp"), P("shard", None), P(None, "tp"),
        P("shard", "tp"), P("shard", None), P(None, "tp"),
        P("shard", "tp"), P("shard", None), P(None, "tp"),
        P(("shard", "tp")), P(("shard", "tp")),
    )
    out_specs = (P("tp", None), P("tp", None), P("tp", None), P())
    return jax.shard_map(per_device, mesh=mesh, in_specs=in_specs, out_specs=out_specs, check_vma=False)
```

```python
import jax
import jax.numpy as jnp
from jax import lax
from jax.experimental import pallas as pl
from jax.experimental.pallas import tpu as pltpu
from jax.sharding import PartitionSpec as P

MESH = pl.DeviceIdType.MESH
mix_rate = 0.5

ROWS, COLS, TILE = 1280, 512, 128
PART = ROWS // 4
SLOTS = 15
A, B, C, D = 0, 1, 2, 3


def schedule():
    def order(first, second, own_first, own_second, step, place):
        side = lambda far: place(0, far)
        return [
            side(0) + (first,), side(0) + (second,), side(0) + (own_first,), side(0) + (own_second,),
            place(-step, 0) + (first,),
            side(-1) + (own_first,), side(-1) + (own_second,),
            place(-step, 0) + (own_first,),
            side(1) + (own_first,), side(1) + (own_second,),
            side(2) + (own_first,), side(2) + (own_second,),
            place(-step, -1) + (own_first,), place(-step, 1) + (own_first,), place(-step, 2) + (own_first,),
        ]

    along_y = lambda along, across: (along, across)
    along_z = lambda along, across: (across, along)
    return (
        ((1, 0), order(A, B, C, D, 1, along_y)),
        ((-1, 0), order(B, A, D, C, -1, along_y)),
        ((0, 1), order(C, D, A, B, 1, along_z)),
        ((0, -1), order(D, C, B, A, -1, along_z)),
    )


AHEAD = 4
BREAK = (14, 11)
LATE = SLOTS - min(BREAK)
LINKS = schedule()
ARRIVALS = [
    [(((dy - ty + 1) % 4) - 1, ((dz - tz + 1) % 4) - 1, part) for dy, dz, part in items] for (ty, tz), items in LINKS
]
PLACE = {ARRIVALS[link][slot]: (link, slot) for link in range(4) for slot in range(SLOTS)}
TILES = (
    (0, ((0, 0, 0, 128), (1, 1, 0, 128))),
    (5, ((2, 0, 640, 128), (3, 1, 640, 128))),
    (4, ((1, 0, 512, 128),)),
    (9, ((3, 0, 1152, 128),)),
    (1, ((0, 0, 128, 128),)),
    (6, ((2, 0, 768, 128),)),
    (3, ((1, 0, 384, 128),)),
    (8, ((3, 0, 1024, 128),)),
    (2, ((0, 0, 256, 64), (1, 0, 320, 64), (1, 1, 128, 192))),
    (7, ((2, 0, 896, 64), (3, 0, 960, 64), (3, 1, 768, 192))),
)


def position():
    shard, core = lax.axis_index("shard"), lax.axis_index("tp") % 2
    z, y = shard // 4, shard % 4

    def at(dy, dz):
        return ((z + dz + 4) % 4) * 4 + (y + dy + 4) % 4

    return shard, core, at


def gather_kernel(
    tq, lq, hq, tk, lk, hk, tv, lv, hv, nt, ns,
    out, norm_out,
    t_in, l_in, h_in, nt_in, ns_in, norm_all, norm_rows,
    load_sem, send_sem, recv_sem, norm_send, norm_recv,
):
    shard, core, at = position()
    tp = lax.axis_index("tp")
    z, x = shard // 4, tp // 2

    def other(dx):
        return ((x + dx + 4) % 4) * 2 + core

    loads = {}

    def load(name, src, dst):
        loads[name] = pltpu.make_async_copy(src, dst, load_sem.at[len(loads)])
        loads[name].start()

    def load_tile(tile):
        if tile < 8:
            load(("t", tile), tq.at[:, pl.ds(tile * TILE, TILE)], t_in.at[tile])
        else:
            load(("t", tile), (tk, tv)[tile - 8], t_in.at[tile])

    load(("l", 0), lq, l_in.at[0])
    load(("h", 0), hq, h_in.at[:, pl.ds(0, 1024)])
    for tile, _ in TILES[:3]:
        load_tile(tile)
    load(("l", 2), lv, l_in.at[2])
    load(("h", 2), hv, h_in.at[:, pl.ds(1152, TILE)])
    for tile, _ in TILES[3:7]:
        load_tile(tile)
    load(("l", 1), lk, l_in.at[1])
    load(("h", 1), hk, h_in.at[:, pl.ds(1024, TILE)])
    for tile, _ in TILES[7:]:
        load_tile(tile)
    load("nt", nt, nt_in)
    load("ns", ns, ns_in)

    barrier = pltpu.get_barrier_semaphore()
    for (dy, dz), _ in LINKS:
        pl.semaphore_signal(barrier, inc=1, device_id={"shard": at(dy, dz)}, device_id_type=MESH)
    for peer in (x * 2 + 1 - core, other(1), other(-1)):
        pl.semaphore_signal(barrier, inc=1, device_id={"tp": peer}, device_id_type=MESH)

    def send(link, slot, rows=None):
        (ty, tz), items = LINKS[link]
        dy, dz, part = items[slot]
        row, count = rows if rows is not None else (part * PART, PART)
        piece = out.at[at(dy, dz), pl.ds(row, count)]
        return pltpu.make_async_remote_copy(
            src_ref=piece, dst_ref=piece, send_sem=send_sem.at[link, slot], recv_sem=recv_sem.at[link, slot],
            device_id={"shard": at(ty, tz)}, device_id_type=MESH,
        )

    def arrival(link, slot):
        (ty, tz), items = LINKS[link]
        dy, dz, part = items[slot]
        piece = out.at[at(dy - ty, dz - tz), pl.ds(part * PART, PART)]
        return pltpu.make_async_remote_copy(
            src_ref=piece, dst_ref=piece, send_sem=send_sem.at[link, slot], recv_sem=recv_sem.at[link, slot],
            device_id={"shard": at(ty, tz)}, device_id_type=MESH,
        )

    def merge(tile):
        loads[("t", tile)].wait()
        which = max(tile - 7, 0)
        for name in (("l", which), ("h", which)):
            if name in loads:
                loads.pop(name).wait()
        product = lax.dot_general(
            h_in[:, tile * TILE:(tile + 1) * TILE], l_in[which], (((0,), (0,)), ((), ())),
            preferred_element_type=jnp.float32,
        )
        whole = t_in[tile].astype(jnp.float32).T + mix_rate * product
        out[shard, tile * TILE:(tile + 1) * TILE, :] = whole.astype(jnp.bfloat16)

    waiting = ()
    for place, (tile, pieces) in enumerate(TILES):
        merge(tile)
        if place == 1:
            pl.semaphore_wait(barrier, 7)
        for link, slot, row, count in waiting:
            send(link, slot, (row, count)).start()
        waiting = pieces
    for link, slot, row, count in waiting:
        send(link, slot, (row, count)).start()
    for link in (0, 2):
        send(link, 1).start()
    for slot in range(2, AHEAD):
        for link in range(4):
            send(link, slot).start()

    loads["nt"].wait()
    loads["ns"].wait()
    gain = nt_in[...] + ns_in[...]
    both = jnp.concatenate([gain, gain], axis=1)
    half = lax.broadcasted_iota(jnp.int32, (1, 128), 1) // 64
    norm_all[shard, tp] = jnp.where(half == core, both, 0.0)

    def norm_copy(step, piece, peer):
        return pltpu.make_async_remote_copy(
            src_ref=piece, dst_ref=piece, send_sem=norm_send.at[step], recv_sem=norm_recv.at[step],
            device_id=peer, device_id_type=MESH,
        )

    def pair(dx):
        return norm_all.at[shard, pl.ds(((x + dx + 4) % 4) * 2, 2)]

    def row_of(dy):
        return norm_all.at[at(dy, 0)]

    def plane_of(dz):
        return norm_all.at[pl.ds(((z + dz + 4) % 4) * 4, 4)]

    own = norm_all.at[shard, tp]
    twin = norm_all.at[shard, x * 2 + 1 - core]
    norm_steps = (
        ((0, own, {"tp": x * 2 + 1 - core}, twin),),
        ((1, pair(0), {"tp": other(1)}, pair(-1)), (2, pair(0), {"tp": other(-1)}, pair(1))),
        ((3, pair(-1), {"tp": other(1)}, pair(2)),),
        ((4, row_of(0), {"shard": at(1, 0)}, row_of(-1)), (5, row_of(0), {"shard": at(-1, 0)}, row_of(1))),
        ((6, row_of(-1), {"shard": at(1, 0)}, row_of(2)),),
        ((7, plane_of(0), {"shard": at(0, 1)}, plane_of(-1)), (8, plane_of(0), {"shard": at(0, -1)}, plane_of(1))),
        ((9, plane_of(-1), {"shard": at(0, 1)}, plane_of(2)),),
    )

    def norm_start(step):
        for sem, sent, peer, _ in norm_steps[step]:
            norm_copy(sem, sent, peer).start()

    def norm_wait(step):
        for sem, sent, peer, arrived in norm_steps[step]:
            norm_copy(sem, sent, peer).wait_send()
            norm_copy(sem, arrived, peer).wait_recv()

    def launch(slot):
        for link in range(4):
            send(link, slot).start()

    def receive(slot):
        for link in range(4):
            arrival(link, slot).wait_recv()

    def sent(slots):
        for slot in slots:
            for link in range(4):
                send(link, slot).wait_send()

    norm_start(0)
    first, last = min(BREAK), max(BREAK)
    later = core == BREAK.index(last)
    for slot in range(first):
        receive(slot)
        if slot < len(norm_steps):
            norm_wait(slot)
        if slot + 1 < len(norm_steps):
            norm_start(slot + 1)
        if slot + AHEAD < first:
            launch(slot + AHEAD)
        elif slot + AHEAD < last:
            pl.when(later)(lambda: launch(slot + AHEAD))
        if slot == len(norm_steps):
            for row in range(64):
                even = norm_all[row // 4, (row % 4) * 2]
                odd = norm_all[row // 4, (row % 4) * 2 + 1]
                norm_rows[row:row + 1, :] = even + odd
            norm_out[...] = norm_rows[...].astype(jnp.bfloat16)

    @pl.when(later)
    def _():
        for slot in range(first, last):
            receive(slot)
            if slot + AHEAD < last:
                launch(slot + AHEAD)
        sent(range(first, last))

    sent(range(first))


def rest_kernel(block, norm, rest, send_sem, recv_sem):
    _, core, at = position()
    barrier = pltpu.get_barrier_semaphore()
    for (dy, dz), _ in LINKS:
        pl.semaphore_signal(barrier, inc=1, device_id={"shard": at(dy, dz)}, device_id_type=MESH)
    pl.semaphore_wait(barrier, 4)

    def run(first):
        def copy(link, slot):
            (ty, tz), items = LINKS[link]
            dy, dz, part = items[slot]
            from_link, from_slot = PLACE.get(((dy + 1) % 4 - 1, (dz + 1) % 4 - 1, part), (0, -1))
            if from_slot < first:
                piece = block.at[at(dy, dz), pl.ds(part * PART, PART)]
            else:
                piece = rest.at[from_link, from_slot - first]
            return pltpu.make_async_remote_copy(
                src_ref=piece, dst_ref=rest.at[link, slot - first],
                send_sem=send_sem.at[link, slot - first], recv_sem=recv_sem.at[link, slot - first],
                device_id={"shard": at(ty, tz)}, device_id_type=MESH,
            )

        for slot in range(first, min(first + AHEAD, SLOTS)):
            for link in range(4):
                copy(link, slot).start()
        for slot in range(first, SLOTS):
            for link in range(4):
                copy(link, slot).wait_recv()
            if slot + AHEAD < SLOTS:
                for link in range(4):
                    copy(link, slot + AHEAD).start()
        for slot in range(first, SLOTS):
            for link in range(4):
                copy(link, slot).wait_send()

    for which in range(2):
        pl.when(core == which)(lambda: run(BREAK[which]))


def write_part(copies, sem, src, owner, part, q, k, v):
    columns = pl.ds(pl.multiple_of(owner * COLS, COLS), COLS)
    row, count = part * PART, min(PART, 1024 - part * PART)
    pieces = [(0, count, q.at[pl.ds(row, count), columns])]
    if part == D:
        pieces += [(64, 128, k.at[:, columns]), (192, 128, v.at[:, columns])]
    for start, rows, dst in pieces:
        copies.append(pltpu.make_async_copy(src.at[pl.ds(start, rows)], dst, sem.at[len(copies)]))
        copies[-1].start()


def write_kernel(block, norm, q, k, v, n, sem):
    shard, core, at = position()

    def run(first):
        copies = []
        for part in range(4):
            for far in range(16):
                dy, dz = far % 4 - 1, far // 4 - 1
                if PLACE.get((dy, dz, part), (0, -1))[1] < first:
                    src = block.at[at(dy, dz), pl.ds(part * PART, PART)]
                    write_part(copies, sem, src, at(dy, dz), part, q, k, v)
        copies.append(pltpu.make_async_copy(norm, n, sem.at[len(copies)]))
        copies[-1].start()
        for c in copies:
            c.wait()

    for which in range(2):
        pl.when(core == which)(lambda: run(BREAK[which]))


def write_rest_kernel(rest, q_in, k_in, v_in, q, k, v, sem):
    _, core, at = position()

    def run(first):
        copies = []
        for (dy, dz, part), (link, slot) in PLACE.items():
            if slot >= first:
                write_part(copies, sem, rest.at[link, slot - first], at(dy, dz), part, q, k, v)
        for c in copies:
            c.wait()

    for which in range(2):
        pl.when(core == which)(lambda: run(BREAK[which]))


def per_device(tq, lq, hq, tk, lk, hk, tv, lv, hv, nt, ns):
    hbm = pl.BlockSpec(memory_space=pltpu.HBM)
    vmem = pl.BlockSpec(memory_space=pltpu.VMEM)
    bf16, f32 = jnp.bfloat16, jnp.float32
    block, norm = pl.pallas_call(
        gather_kernel,
        out_shape=(pltpu.VMEM((16, ROWS, COLS), bf16), pltpu.VMEM((64, 128), bf16)),
        in_specs=[hbm] * 11,
        out_specs=(vmem, vmem),
        scratch_shapes=[
            pltpu.VMEM((10, COLS, TILE), bf16),
            pltpu.VMEM((3, 16, COLS), bf16),
            pltpu.VMEM((16, ROWS), bf16),
            pltpu.VMEM((1, 64), f32),
            pltpu.VMEM((1, 64), f32),
            pltpu.VMEM((16, 8, 1, 128), f32),
            pltpu.VMEM((64, 128), f32),
            pltpu.SemaphoreType.DMA((18,)),
            pltpu.SemaphoreType.DMA((4, SLOTS)),
            pltpu.SemaphoreType.DMA((4, SLOTS)),
            pltpu.SemaphoreType.DMA((10,)),
            pltpu.SemaphoreType.DMA((10,)),
        ],
        compiler_params=pltpu.CompilerParams(
            collective_id=0, has_side_effects=True, vmem_limit_bytes=12 * 1024 * 1024
        ),
        name="gather",
    )(*(
        pltpu.with_memory_space_constraint(a, pltpu.HBM)
        for a in (tq, lq.T, hq, tk, lk.T, hk, tv, lv.T, hv, nt.reshape(1, 64), ns.reshape(1, 64))
    ))
    results = (
        jax.ShapeDtypeStruct((1024, 8192), bf16),
        jax.ShapeDtypeStruct((128, 8192), bf16),
        jax.ShapeDtypeStruct((128, 8192), bf16),
    )
    q, k, v, n = pl.pallas_call(
        write_kernel,
        out_shape=results + (jax.ShapeDtypeStruct((64, 128), bf16),),
        in_specs=[vmem, vmem],
        out_specs=(hbm,) * 4,
        scratch_shapes=[pltpu.SemaphoreType.DMA((100,))],
        compiler_params=pltpu.CompilerParams(vmem_limit_bytes=4 * 1024 * 1024),
        name="write",
    )(block, norm)
    rest = pl.pallas_call(
        rest_kernel,
        out_shape=pltpu.VMEM((4, LATE, PART, COLS), bf16),
        in_specs=[vmem, hbm],
        out_specs=vmem,
        scratch_shapes=[pltpu.SemaphoreType.DMA((4, LATE)), pltpu.SemaphoreType.DMA((4, LATE))],
        compiler_params=pltpu.CompilerParams(
            collective_id=1, has_side_effects=True, vmem_limit_bytes=4 * 1024 * 1024
        ),
        name="rest",
    )(block, pltpu.with_memory_space_constraint(n, pltpu.HBM))
    q, k, v = pl.pallas_call(
        write_rest_kernel,
        out_shape=results,
        in_specs=[vmem] + [hbm] * 3,
        out_specs=(hbm,) * 3,
        input_output_aliases={1: 0, 2: 1, 3: 2},
        scratch_shapes=[pltpu.SemaphoreType.DMA((100,))],
        compiler_params=pltpu.CompilerParams(vmem_limit_bytes=4 * 1024 * 1024),
        name="write_rest",
    )(rest, *(pltpu.with_memory_space_constraint(a, pltpu.HBM) for a in (q, k, v)))
    return q, k, v, n.reshape(8192)


def solution(mesh):
    in_specs = (
        P("shard", "tp"), P("shard", None), P(None, "tp"),
        P("shard", "tp"), P("shard", None), P(None, "tp"),
        P("shard", "tp"), P("shard", None), P(None, "tp"),
        P(("shard", "tp")), P(("shard", "tp")),
    )
    out_specs = (P("tp", None), P("tp", None), P("tp", None), P())
    return jax.shard_map(per_device, mesh=mesh, in_specs=in_specs, out_specs=out_specs, check_vma=False)
```

```python
import jax
import jax.numpy as jnp
from jax import lax
from jax.experimental import pallas as pl
from jax.experimental.pallas import tpu as pltpu
from jax.sharding import PartitionSpec as P

MESH = pl.DeviceIdType.MESH
mix_rate = 0.5

ROWS, COLS, TILE = 1280, 512, 128
PART = ROWS // 4
SLOTS = 15
A, B, C, D = 0, 1, 2, 3


def schedule():
    def order(first, second, own_first, own_second, step, place):
        side = lambda far: place(0, far)
        return [
            side(0) + (first,), side(0) + (second,), side(0) + (own_first,), side(0) + (own_second,),
            place(-step, 0) + (first,),
            side(-1) + (own_first,), side(-1) + (own_second,),
            place(-step, 0) + (own_first,),
            side(1) + (own_first,), side(1) + (own_second,),
            side(2) + (own_first,), side(2) + (own_second,),
            place(-step, -1) + (own_first,), place(-step, 1) + (own_first,), place(-step, 2) + (own_first,),
        ]

    along_y = lambda along, across: (along, across)
    along_z = lambda along, across: (across, along)
    return (
        ((1, 0), order(A, B, C, D, 1, along_y)),
        ((-1, 0), order(B, A, D, C, -1, along_y)),
        ((0, 1), order(C, D, A, B, 1, along_z)),
        ((0, -1), order(D, C, B, A, -1, along_z)),
    )


AHEAD = 4
NORM_AT = {1: 3, 4: 4, 7: 5, 10: 6}
BREAK = (14, 11)
LATE = SLOTS - min(BREAK)
LINKS = schedule()
ARRIVALS = [
    [(((dy - ty + 1) % 4) - 1, ((dz - tz + 1) % 4) - 1, part) for dy, dz, part in items] for (ty, tz), items in LINKS
]
PLACE = {ARRIVALS[link][slot]: (link, slot) for link in range(4) for slot in range(SLOTS)}
TILES = (
    (0, ((0, 0, 0, 128), (1, 1, 0, 128))),
    (5, ((2, 0, 640, 128), (3, 1, 640, 128))),
    (4, ((1, 0, 512, 128),)),
    (9, ((3, 0, 1152, 128),)),
    (1, ((0, 0, 128, 128),)),
    (6, ((2, 0, 768, 128),)),
    (3, ((1, 0, 384, 128),)),
    (8, ((3, 0, 1024, 128),)),
    (2, ((0, 0, 256, 64), (1, 0, 320, 64), (1, 1, 128, 192))),
    (7, ((2, 0, 896, 64), (3, 0, 960, 64), (3, 1, 768, 192))),
)


def position():
    shard, core = lax.axis_index("shard"), lax.axis_index("tp") % 2
    z, y = shard // 4, shard % 4

    def at(dy, dz):
        return ((z + dz + 4) % 4) * 4 + (y + dy + 4) % 4

    return shard, core, at


def gather_kernel(
    tq, lq, hq, tk, lk, hk, tv, lv, hv, nt, ns,
    out, norm_out,
    t_in, l_in, h_in, nt_in, ns_in, norm_all, norm_rows,
    load_sem, send_sem, recv_sem, norm_send, norm_recv,
):
    shard, core, at = position()
    tp = lax.axis_index("tp")
    z, x = shard // 4, tp // 2

    def other(dx):
        return ((x + dx + 4) % 4) * 2 + core

    loads = {}

    def load(name, src, dst):
        loads[name] = pltpu.make_async_copy(src, dst, load_sem.at[len(loads)])
        loads[name].start()

    def load_tile(tile):
        if tile < 8:
            load(("t", tile), tq.at[:, pl.ds(tile * TILE, TILE)], t_in.at[tile])
        else:
            load(("t", tile), (tk, tv)[tile - 8], t_in.at[tile])

    for tile, _ in TILES[:2]:
        load_tile(tile)
    load(("l", 0), lq, l_in.at[0])
    load(("h", 0), hq, h_in.at[:, pl.ds(0, 1024)])
    load("nt", nt, nt_in)
    load("ns", ns, ns_in)

    barrier = pltpu.get_barrier_semaphore()
    for (dy, dz), _ in LINKS:
        pl.semaphore_signal(barrier, inc=1, device_id={"shard": at(dy, dz)}, device_id_type=MESH)
    for peer in (x * 2 + 1 - core, other(1), other(-1)):
        pl.semaphore_signal(barrier, inc=1, device_id={"tp": peer}, device_id_type=MESH)

    for tile, _ in TILES[2:4]:
        load_tile(tile)
    load(("l", 2), lv, l_in.at[2])
    load(("h", 2), hv, h_in.at[:, pl.ds(1152, TILE)])
    load(("l", 1), lk, l_in.at[1])
    load(("h", 1), hk, h_in.at[:, pl.ds(1024, TILE)])
    for tile, _ in TILES[4:]:
        load_tile(tile)

    def send(link, slot, rows=None):
        (ty, tz), items = LINKS[link]
        dy, dz, part = items[slot]
        row, count = rows if rows is not None else (part * PART, PART)
        piece = out.at[at(dy, dz), pl.ds(row, count)]
        return pltpu.make_async_remote_copy(
            src_ref=piece, dst_ref=piece, send_sem=send_sem, recv_sem=recv_sem.at[link, slot],
            device_id={"shard": at(ty, tz)}, device_id_type=MESH,
        )

    def arrival(link, slot):
        (ty, tz), items = LINKS[link]
        dy, dz, part = items[slot]
        piece = out.at[at(dy - ty, dz - tz), pl.ds(part * PART, PART)]
        return pltpu.make_async_remote_copy(
            src_ref=piece, dst_ref=piece, send_sem=send_sem, recv_sem=recv_sem.at[link, slot],
            device_id={"shard": at(ty, tz)}, device_id_type=MESH,
        )

    def merge(tile):
        loads[("t", tile)].wait()
        which = max(tile - 7, 0)
        for name in (("l", which), ("h", which)):
            if name in loads:
                loads.pop(name).wait()
        product = lax.dot_general(
            h_in[:, tile * TILE:(tile + 1) * TILE], l_in[which], (((0,), (0,)), ((), ())),
            preferred_element_type=jnp.float32,
        )
        whole = t_in[tile].astype(jnp.float32).T + mix_rate * product
        out[shard, tile * TILE:(tile + 1) * TILE, :] = whole.astype(jnp.bfloat16)

    waiting = ()
    for place, (tile, pieces) in enumerate(TILES):
        merge(tile)
        if place == 1:
            pl.semaphore_wait(barrier, 7)
        for link, slot, row, count in waiting:
            send(link, slot, (row, count)).start()
        waiting = pieces
    for link, slot, row, count in waiting:
        send(link, slot, (row, count)).start()
    for link in (0, 2):
        send(link, 1).start()
    loads["nt"].wait()
    loads["ns"].wait()
    gain = nt_in[...] + ns_in[...]
    both = jnp.concatenate([gain, gain], axis=1)
    half = lax.broadcasted_iota(jnp.int32, (1, 128), 1) // 64
    norm_all[shard, tp] = jnp.where(half == core, both, 0.0)

    def norm_copy(step, piece, peer):
        return pltpu.make_async_remote_copy(
            src_ref=piece, dst_ref=piece, send_sem=norm_send.at[step], recv_sem=norm_recv.at[step],
            device_id=peer, device_id_type=MESH,
        )

    def pair(dx):
        return norm_all.at[shard, pl.ds(((x + dx + 4) % 4) * 2, 2)]

    def row_of(dy):
        return norm_all.at[at(dy, 0)]

    def plane_of(dz):
        return norm_all.at[pl.ds(((z + dz + 4) % 4) * 4, 4)]

    own = norm_all.at[shard, tp]
    twin = norm_all.at[shard, x * 2 + 1 - core]
    norm_steps = (
        ((0, own, {"tp": x * 2 + 1 - core}, twin),),
        ((1, pair(0), {"tp": other(1)}, pair(-1)), (2, pair(0), {"tp": other(-1)}, pair(1))),
        ((3, pair(-1), {"tp": other(1)}, pair(2)),),
        ((4, row_of(0), {"shard": at(1, 0)}, row_of(-1)), (5, row_of(0), {"shard": at(-1, 0)}, row_of(1))),
        ((6, row_of(-1), {"shard": at(1, 0)}, row_of(2)),),
        ((7, plane_of(0), {"shard": at(0, 1)}, plane_of(-1)), (8, plane_of(0), {"shard": at(0, -1)}, plane_of(1))),
        ((9, plane_of(-1), {"shard": at(0, 1)}, plane_of(2)),),
    )

    def norm_start(step):
        for sem, sent, peer, _ in norm_steps[step]:
            norm_copy(sem, sent, peer).start()

    def norm_wait(step):
        for sem, sent, peer, arrived in norm_steps[step]:
            norm_copy(sem, sent, peer).wait_send()
            norm_copy(sem, arrived, peer).wait_recv()

    def launch(slot):
        for link in range(4):
            send(link, slot).start()

    def receive(slot):
        for link in range(4):
            arrival(link, slot).wait_recv()

    def sent(slots):
        blocks = out.at[pl.ds(0, slots)]
        pltpu.make_async_copy(blocks, blocks, send_sem).wait()

    norm_start(0)
    for step in range(3):
        norm_wait(step)
        norm_start(step + 1)
    for slot in range(2, AHEAD):
        launch(slot)
    first, last = min(BREAK), max(BREAK)
    later = core == BREAK.index(last)
    for slot in range(first):
        receive(slot)
        if slot in NORM_AT:
            norm_wait(NORM_AT[slot])
            if NORM_AT[slot] + 1 < len(norm_steps):
                norm_start(NORM_AT[slot] + 1)
        if slot + AHEAD < first:
            launch(slot + AHEAD)
        elif slot + AHEAD < last:
            pl.when(later)(lambda: launch(slot + AHEAD))
        if slot == max(NORM_AT):
            for row in range(64):
                even = norm_all[row // 4, (row % 4) * 2]
                odd = norm_all[row // 4, (row % 4) * 2 + 1]
                norm_rows[row:row + 1, :] = even + odd
            norm_out[...] = norm_rows[...].astype(jnp.bfloat16)

    @pl.when(later)
    def _():
        for slot in range(first, last):
            receive(slot)
            if slot + AHEAD < last:
                launch(slot + AHEAD)
        sent(last)

    @pl.when(jnp.logical_not(later))
    def _():
        sent(first)


def rest_kernel(block, norm, rest, send_sem, recv_sem):
    _, core, at = position()
    barrier = pltpu.get_barrier_semaphore()
    for (dy, dz), _ in LINKS:
        pl.semaphore_signal(barrier, inc=1, device_id={"shard": at(dy, dz)}, device_id_type=MESH)
    pl.semaphore_wait(barrier, 4)

    def run(first):
        def copy(link, slot):
            (ty, tz), items = LINKS[link]
            dy, dz, part = items[slot]
            from_link, from_slot = PLACE.get(((dy + 1) % 4 - 1, (dz + 1) % 4 - 1, part), (0, -1))
            if from_slot < first:
                piece = block.at[at(dy, dz), pl.ds(part * PART, PART)]
            else:
                piece = rest.at[from_link, from_slot - first]
            return pltpu.make_async_remote_copy(
                src_ref=piece, dst_ref=rest.at[link, slot - first],
                send_sem=send_sem, recv_sem=recv_sem.at[link, slot - first],
                device_id={"shard": at(ty, tz)}, device_id_type=MESH,
            )

        for slot in range(first, min(first + AHEAD, SLOTS)):
            for link in range(4):
                copy(link, slot).start()
        for slot in range(first, SLOTS):
            for link in range(4):
                copy(link, slot).wait_recv()
            if slot + AHEAD < SLOTS:
                for link in range(4):
                    copy(link, slot + AHEAD).start()
        sent = rest.at[:, pl.ds(0, SLOTS - first)]
        pltpu.make_async_copy(sent, sent, send_sem).wait()

    for which in range(2):
        pl.when(core == which)(lambda: run(BREAK[which]))


def write_part(sem, src, owner, part, q, k, v):
    columns = pl.ds(pl.multiple_of(owner * COLS, COLS), COLS)
    row, count = part * PART, min(PART, 1024 - part * PART)
    pieces = [(0, count, q.at[pl.ds(row, count), columns])]
    if part == D:
        pieces += [(64, 128, k.at[:, columns]), (192, 128, v.at[:, columns])]
    for start, rows, dst in pieces:
        pltpu.make_async_copy(src.at[pl.ds(start, rows)], dst, sem).start()


def write_kernel(block, norm, q, k, v, n, sem, norm_sem):
    _, core, at = position()
    norm_copy = pltpu.make_async_copy(norm, n, norm_sem)
    norm_copy.start()

    def run(first):
        for part in range(4):
            for far in range(16):
                dy, dz = far % 4 - 1, far // 4 - 1
                if PLACE.get((dy, dz, part), (0, -1))[1] < first:
                    src = block.at[at(dy, dz), pl.ds(part * PART, PART)]
                    write_part(sem, src, at(dy, dz), part, q, k, v)
        blocks = block.at[pl.ds(0, 1 + first)]
        pltpu.make_async_copy(blocks, blocks, sem).wait()

    for which in range(2):
        pl.when(core == which)(lambda: run(BREAK[which]))
    norm_copy.wait()


def write_rest_kernel(rest, q_in, k_in, v_in, q, k, v, sem):
    _, core, at = position()

    def run(first):
        for (dy, dz, part), (link, slot) in PLACE.items():
            if slot >= first:
                write_part(sem, rest.at[link, slot - first], at(dy, dz), part, q, k, v)
        parts = rest.at[:, pl.ds(0, SLOTS - first)]
        pltpu.make_async_copy(parts, parts, sem).wait()

    for which in range(2):
        pl.when(core == which)(lambda: run(BREAK[which]))


def per_device(tq, lq, hq, tk, lk, hk, tv, lv, hv, nt, ns):
    hbm = pl.BlockSpec(memory_space=pltpu.HBM)
    vmem = pl.BlockSpec(memory_space=pltpu.VMEM)
    bf16, f32 = jnp.bfloat16, jnp.float32
    block, norm = pl.pallas_call(
        gather_kernel,
        out_shape=(pltpu.VMEM((16, ROWS, COLS), bf16), pltpu.VMEM((64, 128), bf16)),
        in_specs=[hbm] * 11,
        out_specs=(vmem, vmem),
        scratch_shapes=[
            pltpu.VMEM((10, COLS, TILE), bf16),
            pltpu.VMEM((3, 16, COLS), bf16),
            pltpu.VMEM((16, ROWS), bf16),
            pltpu.VMEM((1, 64), f32),
            pltpu.VMEM((1, 64), f32),
            pltpu.VMEM((16, 8, 1, 128), f32),
            pltpu.VMEM((64, 128), f32),
            pltpu.SemaphoreType.DMA((18,)),
            pltpu.SemaphoreType.DMA,
            pltpu.SemaphoreType.DMA((4, SLOTS)),
            pltpu.SemaphoreType.DMA((10,)),
            pltpu.SemaphoreType.DMA((10,)),
        ],
        compiler_params=pltpu.CompilerParams(
            collective_id=0, has_side_effects=True, vmem_limit_bytes=12 * 1024 * 1024
        ),
        name="gather",
    )(*(
        pltpu.with_memory_space_constraint(a, pltpu.HBM)
        for a in (tq, lq.T, hq, tk, lk.T, hk, tv, lv.T, hv, nt.reshape(1, 64), ns.reshape(1, 64))
    ))
    results = (
        jax.ShapeDtypeStruct((1024, 8192), bf16),
        jax.ShapeDtypeStruct((128, 8192), bf16),
        jax.ShapeDtypeStruct((128, 8192), bf16),
    )
    q, k, v, n = pl.pallas_call(
        write_kernel,
        out_shape=results + (jax.ShapeDtypeStruct((64, 128), bf16),),
        in_specs=[vmem, vmem],
        out_specs=(hbm,) * 4,
        scratch_shapes=[pltpu.SemaphoreType.DMA, pltpu.SemaphoreType.DMA],
        compiler_params=pltpu.CompilerParams(vmem_limit_bytes=4 * 1024 * 1024),
        name="write",
    )(block, norm)
    rest = pl.pallas_call(
        rest_kernel,
        out_shape=pltpu.VMEM((4, LATE, PART, COLS), bf16),
        in_specs=[vmem, hbm],
        out_specs=vmem,
        scratch_shapes=[pltpu.SemaphoreType.DMA, pltpu.SemaphoreType.DMA((4, LATE))],
        compiler_params=pltpu.CompilerParams(
            collective_id=1, has_side_effects=True, vmem_limit_bytes=4 * 1024 * 1024
        ),
        name="rest",
    )(block, pltpu.with_memory_space_constraint(n, pltpu.HBM))
    q, k, v = pl.pallas_call(
        write_rest_kernel,
        out_shape=results,
        in_specs=[vmem] + [hbm] * 3,
        out_specs=(hbm,) * 3,
        input_output_aliases={1: 0, 2: 1, 3: 2},
        scratch_shapes=[pltpu.SemaphoreType.DMA],
        compiler_params=pltpu.CompilerParams(vmem_limit_bytes=4 * 1024 * 1024),
        name="write_rest",
    )(rest, *(pltpu.with_memory_space_constraint(a, pltpu.HBM) for a in (q, k, v)))
    return q, k, v, n.reshape(8192)


def solution(mesh):
    in_specs = (
        P("shard", "tp"), P("shard", None), P(None, "tp"),
        P("shard", "tp"), P("shard", None), P(None, "tp"),
        P("shard", "tp"), P("shard", None), P(None, "tp"),
        P(("shard", "tp")), P(("shard", "tp")),
    )
    out_specs = (P("tp", None), P("tp", None), P("tp", None), P())
    return jax.shard_map(per_device, mesh=mesh, in_specs=in_specs, out_specs=out_specs, check_vma=False)
```

```python
import jax
import jax.numpy as jnp
from jax import lax
from jax.experimental import pallas as pl
from jax.experimental.pallas import tpu as pltpu
from jax.sharding import PartitionSpec as P

MESH = pl.DeviceIdType.MESH
mix_rate = 0.5

ROWS, COLS, TILE = 1280, 512, 128
PART = ROWS // 4
SLOTS = 15
A, B, C, D = 0, 1, 2, 3


def schedule():
    def order(first, second, own_first, own_second, step, place):
        side = lambda far: place(0, far)
        return [
            side(0) + (first,), side(0) + (second,), side(0) + (own_first,), side(0) + (own_second,),
            place(-step, 0) + (first,),
            side(-1) + (own_first,), side(-1) + (own_second,),
            place(-step, 0) + (own_first,),
            side(1) + (own_first,), side(1) + (own_second,),
            side(2) + (own_first,), side(2) + (own_second,),
            place(-step, -1) + (own_first,), place(-step, 1) + (own_first,), place(-step, 2) + (own_first,),
        ]

    along_y = lambda along, across: (along, across)
    along_z = lambda along, across: (across, along)
    return (
        ((1, 0), order(A, B, C, D, 1, along_y)),
        ((-1, 0), order(B, A, D, C, -1, along_y)),
        ((0, 1), order(C, D, A, B, 1, along_z)),
        ((0, -1), order(D, C, B, A, -1, along_z)),
    )


AHEAD = 4
NORM_AT = {1: 3, 4: 4, 7: 5, 10: 6}
BREAK = (14, 11)
LATE = SLOTS - min(BREAK)
LINKS = schedule()
ARRIVALS = [
    [(((dy - ty + 1) % 4) - 1, ((dz - tz + 1) % 4) - 1, part) for dy, dz, part in items] for (ty, tz), items in LINKS
]
PLACE = {ARRIVALS[link][slot]: (link, slot) for link in range(4) for slot in range(SLOTS)}
TILES = (
    (0, ((0, 0, 0, 128), (1, 1, 0, 128))),
    (5, ((2, 0, 640, 128), (3, 1, 640, 128))),
    (4, ((1, 0, 512, 128),)),
    (9, ((3, 0, 1152, 128),)),
    (1, ((0, 0, 128, 128),)),
    (6, ((2, 0, 768, 128),)),
    (3, ((1, 0, 384, 128),)),
    (8, ((3, 0, 1024, 128),)),
    (2, ((0, 0, 256, 64), (1, 0, 320, 64), (1, 1, 128, 192))),
    (7, ((2, 0, 896, 64), (3, 0, 960, 64), (3, 1, 768, 192))),
)


def position():
    shard, core = lax.axis_index("shard"), lax.axis_index("tp") % 2
    z, y = shard // 4, shard % 4

    def at(dy, dz):
        return ((z + dz + 4) % 4) * 4 + (y + dy + 4) % 4

    return shard, core, at


def gather_kernel(
    tq, lq, hq, tk, lk, hk, tv, lv, hv, nt, ns,
    out, norm_out,
    t_in, l_in, h_in, nt_in, ns_in, norm_all, norm_rows,
    load_sem, send_sem, recv_sem, norm_send, norm_recv, ready,
):
    shard, core, at = position()
    tp = lax.axis_index("tp")
    z, x = shard // 4, tp // 2

    def other(dx):
        return ((x + dx + 4) % 4) * 2 + core

    loads = {}

    def load(name, src, dst):
        loads[name] = pltpu.make_async_copy(src, dst, load_sem.at[len(loads)])
        loads[name].start()

    def load_tile(tile):
        if tile < 8:
            load(("t", tile), tq.at[:, pl.ds(tile * TILE, TILE)], t_in.at[tile])
        else:
            load(("t", tile), (tk, tv)[tile - 8], t_in.at[tile])

    for tile, _ in TILES[:2]:
        load_tile(tile)
    load(("l", 0), lq, l_in.at[0])
    load(("h", 0), hq, h_in.at[:, pl.ds(0, 1024)])
    load("nt", nt, nt_in)
    load("ns", ns, ns_in)

    y = shard % 4
    peers = [{"shard": at(dy, dz)} for (dy, dz), _ in LINKS]
    peers += [{"tp": x * 2 + 1 - core}, {"tp": other(1)}, {"tp": other(-1)}]
    mirror = (1, 0, 3, 2, 4, 6, 5)
    later = (y < 3, y == 0, z < 3, z == 0, core == 1, x < 3, x == 0)
    barrier = pltpu.get_barrier_semaphore()
    earlier_ones = 7
    for who, peer in enumerate(peers):
        earlier_ones = earlier_ones - later[who].astype(jnp.int32)

        @pl.when(later[who])
        def _():
            pl.semaphore_signal(barrier, inc=1, device_id=peer, device_id_type=MESH)

    for tile, _ in TILES[2:4]:
        load_tile(tile)
    load(("l", 2), lv, l_in.at[2])
    load(("h", 2), hv, h_in.at[:, pl.ds(1152, TILE)])
    load(("l", 1), lk, l_in.at[1])
    load(("h", 1), hk, h_in.at[:, pl.ds(1024, TILE)])
    for tile, _ in TILES[4:]:
        load_tile(tile)

    pl.when(earlier_ones > 0)(lambda: pl.semaphore_wait(barrier, earlier_ones))
    for who, peer in enumerate(peers):

        @pl.when(jnp.logical_not(later[who]))
        def _():
            pl.semaphore_signal(ready.at[mirror[who]], inc=1, device_id=peer, device_id_type=MESH)

    def greet(who):
        @pl.when(later[who])
        def _():
            pl.semaphore_wait(ready.at[who], 1)

    def send(link, slot, rows=None):
        (ty, tz), items = LINKS[link]
        dy, dz, part = items[slot]
        row, count = rows if rows is not None else (part * PART, PART)
        piece = out.at[at(dy, dz), pl.ds(row, count)]
        return pltpu.make_async_remote_copy(
            src_ref=piece, dst_ref=piece, send_sem=send_sem, recv_sem=recv_sem.at[link, slot],
            device_id={"shard": at(ty, tz)}, device_id_type=MESH,
        )

    def arrival(link, slot):
        (ty, tz), items = LINKS[link]
        dy, dz, part = items[slot]
        piece = out.at[at(dy - ty, dz - tz), pl.ds(part * PART, PART)]
        return pltpu.make_async_remote_copy(
            src_ref=piece, dst_ref=piece, send_sem=send_sem, recv_sem=recv_sem.at[link, slot],
            device_id={"shard": at(ty, tz)}, device_id_type=MESH,
        )

    def merge(tile):
        loads[("t", tile)].wait()
        which = max(tile - 7, 0)
        for name in (("l", which), ("h", which)):
            if name in loads:
                loads.pop(name).wait()
        product = lax.dot_general(
            h_in[:, tile * TILE:(tile + 1) * TILE], l_in[which], (((0,), (0,)), ((), ())),
            preferred_element_type=jnp.float32,
        )
        whole = t_in[tile].astype(jnp.float32).T + mix_rate * product
        out[shard, tile * TILE:(tile + 1) * TILE, :] = whole.astype(jnp.bfloat16)

    def send_pieces(pieces):
        for link, slot, row, count in pieces:
            pl.when(jnp.logical_not(later[link]))(lambda: send(link, slot, (row, count)).start())

    waiting = ()
    for tile, pieces in TILES:
        merge(tile)
        send_pieces(waiting)
        waiting = pieces

    loads["nt"].wait()
    loads["ns"].wait()
    gain = nt_in[...] + ns_in[...]
    both = jnp.concatenate([gain, gain], axis=1)
    half = lax.broadcasted_iota(jnp.int32, (1, 128), 1) // 64
    norm_all[shard, tp] = jnp.where(half == core, both, 0.0)

    send_pieces(waiting)
    for link in (0, 2):
        pl.when(jnp.logical_not(later[link]))(lambda: send(link, 1).start())
    for link in (0, 2, 1, 3):

        @pl.when(later[link])
        def _():
            pl.semaphore_wait(ready.at[link], 1)
            send(link, 0).start()
            send(link, 1).start()

    for who in (4, 5, 6):
        greet(who)

    def norm_copy(step, piece, peer):
        return pltpu.make_async_remote_copy(
            src_ref=piece, dst_ref=piece, send_sem=norm_send.at[step], recv_sem=norm_recv.at[step],
            device_id=peer, device_id_type=MESH,
        )

    def pair(dx):
        return norm_all.at[shard, pl.ds(((x + dx + 4) % 4) * 2, 2)]

    def row_of(dy):
        return norm_all.at[at(dy, 0)]

    def plane_of(dz):
        return norm_all.at[pl.ds(((z + dz + 4) % 4) * 4, 4)]

    own = norm_all.at[shard, tp]
    twin = norm_all.at[shard, x * 2 + 1 - core]
    norm_steps = (
        ((0, own, {"tp": x * 2 + 1 - core}, twin),),
        ((1, pair(0), {"tp": other(1)}, pair(-1)), (2, pair(0), {"tp": other(-1)}, pair(1))),
        ((3, pair(-1), {"tp": other(1)}, pair(2)),),
        ((4, row_of(0), {"shard": at(1, 0)}, row_of(-1)), (5, row_of(0), {"shard": at(-1, 0)}, row_of(1))),
        ((6, row_of(-1), {"shard": at(1, 0)}, row_of(2)),),
        ((7, plane_of(0), {"shard": at(0, 1)}, plane_of(-1)), (8, plane_of(0), {"shard": at(0, -1)}, plane_of(1))),
        ((9, plane_of(-1), {"shard": at(0, 1)}, plane_of(2)),),
    )

    def norm_start(step):
        for sem, sent, peer, _ in norm_steps[step]:
            norm_copy(sem, sent, peer).start()

    def norm_wait(step):
        for sem, sent, peer, arrived in norm_steps[step]:
            norm_copy(sem, sent, peer).wait_send()
            norm_copy(sem, arrived, peer).wait_recv()

    def launch(slot):
        for link in range(4):
            send(link, slot).start()

    def receive(slot):
        for link in range(4):
            arrival(link, slot).wait_recv()

    def sent(slots):
        blocks = out.at[pl.ds(0, slots)]
        pltpu.make_async_copy(blocks, blocks, send_sem).wait()

    norm_start(0)
    for step in range(3):
        norm_wait(step)
        norm_start(step + 1)
    for slot in range(2, AHEAD):
        launch(slot)
    first, last = min(BREAK), max(BREAK)
    breaks_late = core == BREAK.index(last)
    for slot in range(first):
        receive(slot)
        if slot in NORM_AT:
            norm_wait(NORM_AT[slot])
            if NORM_AT[slot] + 1 < len(norm_steps):
                norm_start(NORM_AT[slot] + 1)
        if slot + AHEAD < first:
            launch(slot + AHEAD)
        elif slot + AHEAD < last:
            pl.when(breaks_late)(lambda: launch(slot + AHEAD))
        if slot == max(NORM_AT):
            for row in range(64):
                even = norm_all[row // 4, (row % 4) * 2]
                odd = norm_all[row // 4, (row % 4) * 2 + 1]
                norm_rows[row:row + 1, :] = even + odd
            norm_out[...] = norm_rows[...].astype(jnp.bfloat16)

    @pl.when(breaks_late)
    def _():
        for slot in range(first, last):
            receive(slot)
            if slot + AHEAD < last:
                launch(slot + AHEAD)
        sent(last)

    @pl.when(jnp.logical_not(breaks_late))
    def _():
        sent(first)


def rest_kernel(block, norm, rest, send_sem, recv_sem, ready):
    shard, core, at = position()
    z, y = shard // 4, shard % 4
    later = (y < 3, y == 0, z < 3, z == 0)
    barrier = pltpu.get_barrier_semaphore()
    earlier_ones = 4
    for link, ((dy, dz), _) in enumerate(LINKS):
        earlier_ones = earlier_ones - later[link].astype(jnp.int32)

        @pl.when(later[link])
        def _():
            pl.semaphore_signal(barrier, inc=1, device_id={"shard": at(dy, dz)}, device_id_type=MESH)

    pl.when(earlier_ones > 0)(lambda: pl.semaphore_wait(barrier, earlier_ones))
    for link, ((dy, dz), _) in enumerate(LINKS):

        @pl.when(jnp.logical_not(later[link]))
        def _():
            pl.semaphore_signal(ready.at[link ^ 1], inc=1, device_id={"shard": at(dy, dz)}, device_id_type=MESH)

    def run(first):
        def copy(link, slot):
            (ty, tz), items = LINKS[link]
            dy, dz, part = items[slot]
            from_link, from_slot = PLACE.get(((dy + 1) % 4 - 1, (dz + 1) % 4 - 1, part), (0, -1))
            if from_slot < first:
                piece = block.at[at(dy, dz), pl.ds(part * PART, PART)]
            else:
                piece = rest.at[from_link, from_slot - first]
            return pltpu.make_async_remote_copy(
                src_ref=piece, dst_ref=rest.at[link, slot - first],
                send_sem=send_sem, recv_sem=recv_sem.at[link, slot - first],
                device_id={"shard": at(ty, tz)}, device_id_type=MESH,
            )

        def launch(link):
            for slot in range(first, SLOTS):
                copy(link, slot).start()

        for link in range(4):
            pl.when(jnp.logical_not(later[link]))(lambda: launch(link))
        for link in (0, 2, 1, 3):

            @pl.when(later[link])
            def _():
                pl.semaphore_wait(ready.at[link], 1)
                launch(link)

        for slot in range(first, SLOTS):
            for link in range(4):
                copy(link, slot).wait_recv()
        sent = rest.at[:, pl.ds(0, SLOTS - first)]
        pltpu.make_async_copy(sent, sent, send_sem).wait()

    for which in range(2):
        pl.when(core == which)(lambda: run(BREAK[which]))


def write_part(sem, src, owner, part, q, k, v):
    columns = pl.ds(pl.multiple_of(owner * COLS, COLS), COLS)
    row, count = part * PART, min(PART, 1024 - part * PART)
    pieces = [(0, count, q.at[pl.ds(row, count), columns])]
    if part == D:
        pieces += [(64, 128, k.at[:, columns]), (192, 128, v.at[:, columns])]
    for start, rows, dst in pieces:
        pltpu.make_async_copy(src.at[pl.ds(start, rows)], dst, sem).start()


def write_kernel(block, norm, q, k, v, n, sem, norm_sem):
    _, core, at = position()
    norm_copy = pltpu.make_async_copy(norm, n, norm_sem)
    norm_copy.start()

    def run(first):
        for part in range(4):
            for far in range(16):
                dy, dz = far % 4 - 1, far // 4 - 1
                if PLACE.get((dy, dz, part), (0, -1))[1] < first:
                    src = block.at[at(dy, dz), pl.ds(part * PART, PART)]
                    write_part(sem, src, at(dy, dz), part, q, k, v)
        blocks = block.at[pl.ds(0, 1 + first)]
        pltpu.make_async_copy(blocks, blocks, sem).wait()

    for which in range(2):
        pl.when(core == which)(lambda: run(BREAK[which]))
    norm_copy.wait()


def write_rest_kernel(rest, q_in, k_in, v_in, q, k, v, sem):
    _, core, at = position()

    def run(first):
        for (dy, dz, part), (link, slot) in PLACE.items():
            if slot >= first:
                write_part(sem, rest.at[link, slot - first], at(dy, dz), part, q, k, v)
        parts = rest.at[:, pl.ds(0, SLOTS - first)]
        pltpu.make_async_copy(parts, parts, sem).wait()

    for which in range(2):
        pl.when(core == which)(lambda: run(BREAK[which]))


def per_device(tq, lq, hq, tk, lk, hk, tv, lv, hv, nt, ns):
    hbm = pl.BlockSpec(memory_space=pltpu.HBM)
    vmem = pl.BlockSpec(memory_space=pltpu.VMEM)
    bf16, f32 = jnp.bfloat16, jnp.float32
    block, norm = pl.pallas_call(
        gather_kernel,
        out_shape=(pltpu.VMEM((16, ROWS, COLS), bf16), pltpu.VMEM((64, 128), bf16)),
        in_specs=[hbm] * 11,
        out_specs=(vmem, vmem),
        scratch_shapes=[
            pltpu.VMEM((10, COLS, TILE), bf16),
            pltpu.VMEM((3, 16, COLS), bf16),
            pltpu.VMEM((16, ROWS), bf16),
            pltpu.VMEM((1, 64), f32),
            pltpu.VMEM((1, 64), f32),
            pltpu.VMEM((16, 8, 1, 128), f32),
            pltpu.VMEM((64, 128), f32),
            pltpu.SemaphoreType.DMA((18,)),
            pltpu.SemaphoreType.DMA,
            pltpu.SemaphoreType.DMA((4, SLOTS)),
            pltpu.SemaphoreType.DMA((10,)),
            pltpu.SemaphoreType.DMA((10,)),
            pltpu.SemaphoreType.REGULAR((7,)),
        ],
        compiler_params=pltpu.CompilerParams(
            collective_id=0, has_side_effects=True, vmem_limit_bytes=12 * 1024 * 1024
        ),
        name="gather",
    )(*(
        pltpu.with_memory_space_constraint(a, pltpu.HBM)
        for a in (tq, lq.T, hq, tk, lk.T, hk, tv, lv.T, hv, nt.reshape(1, 64), ns.reshape(1, 64))
    ))
    results = (
        jax.ShapeDtypeStruct((1024, 8192), bf16),
        jax.ShapeDtypeStruct((128, 8192), bf16),
        jax.ShapeDtypeStruct((128, 8192), bf16),
    )
    q, k, v, n = pl.pallas_call(
        write_kernel,
        out_shape=results + (jax.ShapeDtypeStruct((64, 128), bf16),),
        in_specs=[vmem, vmem],
        out_specs=(hbm,) * 4,
        scratch_shapes=[pltpu.SemaphoreType.DMA, pltpu.SemaphoreType.DMA],
        compiler_params=pltpu.CompilerParams(vmem_limit_bytes=4 * 1024 * 1024),
        name="write",
    )(block, norm)
    rest = pl.pallas_call(
        rest_kernel,
        out_shape=pltpu.VMEM((4, LATE, PART, COLS), bf16),
        in_specs=[vmem, hbm],
        out_specs=vmem,
        scratch_shapes=[
            pltpu.SemaphoreType.DMA, pltpu.SemaphoreType.DMA((4, LATE)), pltpu.SemaphoreType.REGULAR((4,))
        ],
        compiler_params=pltpu.CompilerParams(
            collective_id=1, has_side_effects=True, vmem_limit_bytes=4 * 1024 * 1024
        ),
        name="rest",
    )(block, pltpu.with_memory_space_constraint(n, pltpu.HBM))
    q, k, v = pl.pallas_call(
        write_rest_kernel,
        out_shape=results,
        in_specs=[vmem] + [hbm] * 3,
        out_specs=(hbm,) * 3,
        input_output_aliases={1: 0, 2: 1, 3: 2},
        scratch_shapes=[pltpu.SemaphoreType.DMA],
        compiler_params=pltpu.CompilerParams(vmem_limit_bytes=4 * 1024 * 1024),
        name="write_rest",
    )(rest, *(pltpu.with_memory_space_constraint(a, pltpu.HBM) for a in (q, k, v)))
    return q, k, v, n.reshape(8192)


def solution(mesh):
    in_specs = (
        P("shard", "tp"), P("shard", None), P(None, "tp"),
        P("shard", "tp"), P("shard", None), P(None, "tp"),
        P("shard", "tp"), P("shard", None), P(None, "tp"),
        P(("shard", "tp")), P(("shard", "tp")),
    )
    out_specs = (P("tp", None), P("tp", None), P("tp", None), P())
    return jax.shard_map(per_device, mesh=mesh, in_specs=in_specs, out_specs=out_specs, check_vma=False)
```

```python
import jax
import jax.numpy as jnp
from jax import lax
from jax.experimental import pallas as pl
from jax.experimental.pallas import tpu as pltpu
from jax.sharding import PartitionSpec as P

MESH = pl.DeviceIdType.MESH
mix_rate = 0.5

ROWS, COLS, TILE = 1280, 512, 128
PART = ROWS // 4
SLOTS = 15
A, B, C, D = 0, 1, 2, 3


def schedule():
    def order(first, second, own_first, own_second, step, place):
        side = lambda far: place(0, far)
        return [
            side(0) + (first,), side(0) + (second,), side(0) + (own_first,), side(0) + (own_second,),
            place(-step, 0) + (first,),
            side(-1) + (own_first,), side(-1) + (own_second,),
            place(-step, 0) + (own_first,),
            side(1) + (own_first,), side(1) + (own_second,),
            side(2) + (own_first,), side(2) + (own_second,),
            place(-step, -1) + (own_first,), place(-step, 1) + (own_first,), place(-step, 2) + (own_first,),
        ]

    along_y = lambda along, across: (along, across)
    along_z = lambda along, across: (across, along)
    return (
        ((1, 0), order(A, B, C, D, 1, along_y)),
        ((-1, 0), order(B, A, D, C, -1, along_y)),
        ((0, 1), order(C, D, A, B, 1, along_z)),
        ((0, -1), order(D, C, B, A, -1, along_z)),
    )


AHEAD = 4
NORM_AT = {1: 3, 4: 4, 7: 5, 10: 6}
BREAK = (14, 11)
LATE = SLOTS - min(BREAK)
LINKS = schedule()
SHORT, SHIFT = (2, 4), 48
ARRIVALS = [
    [(((dy - ty + 1) % 4) - 1, ((dz - tz + 1) % 4) - 1, part) for dy, dz, part in items] for (ty, tz), items in LINKS
]
PLACE = {ARRIVALS[link][slot]: (link, slot) for link in range(4) for slot in range(SLOTS)}
TILES = (
    (0, ((0, 0, 0, 128), (1, 1, 0, 128))),
    (5, ((2, 0, 640, 128), (3, 1, 640, 128))),
    (4, ((1, 0, 512, 128),)),
    (9, ((3, 0, 1152, 128),)),
    (1, ((0, 0, 128, 128),)),
    (6, ((2, 0, 768, 128),)),
    (3, ((1, 0, 384, 128),)),
    (8, ((3, 0, 1024, 128),)),
    (2, ((0, 0, 256, 64), (1, 0, 320, 64), (1, 1, 128, 192))),
    (7, ((2, 0, 896, 64), (3, 0, 960, 64), (3, 1, 768, 192))),
)


def position():
    shard, core = lax.axis_index("shard"), lax.axis_index("tp") % 2
    z, y = shard // 4, shard % 4

    def at(dy, dz):
        return ((z + dz + 4) % 4) * 4 + (y + dy + 4) % 4

    return shard, core, at


def gather_kernel(
    tq, lq, hq, tk, lk, hk, tv, lv, hv, nt, ns,
    out, norm_out,
    t_in, l_in, h_in, nt_in, ns_in, norm_all, norm_rows,
    load_sem, send_sem, recv_sem, norm_send, norm_recv, ready, shift_sem,
):
    shard, core, at = position()
    tp = lax.axis_index("tp")
    z, x = shard // 4, tp // 2

    def other(dx):
        return ((x + dx + 4) % 4) * 2 + core

    loads = {}

    def load(name, src, dst):
        loads[name] = pltpu.make_async_copy(src, dst, load_sem.at[len(loads)])
        loads[name].start()

    def load_tile(tile):
        if tile < 8:
            load(("t", tile), tq.at[:, pl.ds(tile * TILE, TILE)], t_in.at[tile])
        else:
            load(("t", tile), (tk, tv)[tile - 8], t_in.at[tile])

    for tile, _ in TILES[:2]:
        load_tile(tile)
    load(("l", 0), lq, l_in.at[0])
    load(("h", 0), hq, h_in.at[:, pl.ds(0, 1024)])
    load("nt", nt, nt_in)
    load("ns", ns, ns_in)

    y = shard % 4
    peers = [{"shard": at(dy, dz)} for (dy, dz), _ in LINKS]
    peers += [{"tp": x * 2 + 1 - core}, {"tp": other(1)}, {"tp": other(-1)}]
    mirror = (1, 0, 3, 2, 4, 6, 5)
    later = (y < 3, y == 0, z < 3, z == 0, core == 1, x < 3, x == 0)
    barrier = pltpu.get_barrier_semaphore()
    earlier_ones = 7
    for who, peer in enumerate(peers):
        earlier_ones = earlier_ones - later[who].astype(jnp.int32)

        @pl.when(later[who])
        def _():
            pl.semaphore_signal(barrier, inc=1, device_id=peer, device_id_type=MESH)

    for tile, _ in TILES[2:4]:
        load_tile(tile)
    load(("l", 2), lv, l_in.at[2])
    load(("h", 2), hv, h_in.at[:, pl.ds(1152, TILE)])
    load(("l", 1), lk, l_in.at[1])
    load(("h", 1), hk, h_in.at[:, pl.ds(1024, TILE)])
    for tile, _ in TILES[4:]:
        load_tile(tile)

    pl.when(earlier_ones > 0)(lambda: pl.semaphore_wait(barrier, earlier_ones))
    for who, peer in enumerate(peers):

        @pl.when(jnp.logical_not(later[who]))
        def _():
            pl.semaphore_signal(ready.at[mirror[who]], inc=1, device_id=peer, device_id_type=MESH)

    def greet(who):
        @pl.when(later[who])
        def _():
            pl.semaphore_wait(ready.at[who], 1)

    def copy(link, slot, owner, rows):
        piece = out.at[owner, pl.ds(*rows)]
        (dy, dz), _ = LINKS[link]
        leaves = send_sem.at[2 if (link, slot) == SHORT else (0, 0, 1, 0)[link]]
        return pltpu.make_async_remote_copy(
            src_ref=piece, dst_ref=piece, send_sem=leaves, recv_sem=recv_sem.at[link, slot],
            device_id={"shard": at(dy, dz)}, device_id_type=MESH,
        )

    def send(link, slot, rows=None):
        dy, dz, part = LINKS[link][1][slot]
        return copy(link, slot, at(dy, dz), rows if rows is not None else (part * PART, PART))

    def arrival(link, slot, cut=0):
        (ty, tz), items = LINKS[link]
        dy, dz, part = items[slot]
        return copy(link, slot, at(dy - ty, dz - tz), (part * PART, PART - cut))

    part = LINKS[SHORT[0]][1][SHORT[1]][2]
    cut_rows, shifted_rows = (part * PART, PART - SHIFT), (part * PART + PART - SHIFT, SHIFT)

    def shifted(dz):
        piece = out.at[at(0, dz), pl.ds(*shifted_rows)]
        return pltpu.make_async_remote_copy(
            src_ref=piece, dst_ref=piece, send_sem=shift_sem.at[0], recv_sem=shift_sem.at[1],
            device_id={"shard": at(0, -1)}, device_id_type=MESH,
        )

    def merge(tile):
        loads[("t", tile)].wait()
        which = max(tile - 7, 0)
        for name in (("l", which), ("h", which)):
            if name in loads:
                loads.pop(name).wait()
        product = lax.dot_general(
            h_in[:, tile * TILE:(tile + 1) * TILE], l_in[which], (((0,), (0,)), ((), ())),
            preferred_element_type=jnp.float32,
        )
        whole = t_in[tile].astype(jnp.float32).T + mix_rate * product
        out[shard, tile * TILE:(tile + 1) * TILE, :] = whole.astype(jnp.bfloat16)

    def send_pieces(pieces):
        for link, slot, row, count in pieces:
            pl.when(jnp.logical_not(later[link]))(lambda: send(link, slot, (row, count)).start())

    waiting = ()
    for tile, pieces in TILES:
        merge(tile)
        send_pieces(waiting)
        waiting = pieces

    loads["nt"].wait()
    loads["ns"].wait()
    gain = nt_in[...] + ns_in[...]
    both = jnp.concatenate([gain, gain], axis=1)
    half = lax.broadcasted_iota(jnp.int32, (1, 128), 1) // 64
    norm_all[shard, tp] = jnp.where(half == core, both, 0.0)

    send_pieces(waiting)
    for link in (0, 2):
        pl.when(jnp.logical_not(later[link]))(lambda: send(link, 1).start())
    for link in (0, 2, 1, 3):

        @pl.when(later[link])
        def _():
            pl.semaphore_wait(ready.at[link], 1)
            send(link, 0).start()
            send(link, 1).start()

    for who in (4, 5, 6):
        greet(who)

    def norm_copy(step, piece, peer):
        return pltpu.make_async_remote_copy(
            src_ref=piece, dst_ref=piece, send_sem=norm_send.at[step], recv_sem=norm_recv.at[step],
            device_id=peer, device_id_type=MESH,
        )

    def pair(dx):
        return norm_all.at[shard, pl.ds(((x + dx + 4) % 4) * 2, 2)]

    def row_of(dy):
        return norm_all.at[at(dy, 0)]

    def plane_of(dz):
        return norm_all.at[pl.ds(((z + dz + 4) % 4) * 4, 4)]

    own = norm_all.at[shard, tp]
    twin = norm_all.at[shard, x * 2 + 1 - core]
    norm_steps = (
        ((0, own, {"tp": x * 2 + 1 - core}, twin),),
        ((1, pair(0), {"tp": other(1)}, pair(-1)), (2, pair(0), {"tp": other(-1)}, pair(1))),
        ((3, pair(-1), {"tp": other(1)}, pair(2)),),
        ((4, row_of(0), {"shard": at(1, 0)}, row_of(-1)), (5, row_of(0), {"shard": at(-1, 0)}, row_of(1))),
        ((6, row_of(-1), {"shard": at(1, 0)}, row_of(2)),),
        ((7, plane_of(0), {"shard": at(0, 1)}, plane_of(-1)), (8, plane_of(0), {"shard": at(0, -1)}, plane_of(1))),
        ((9, plane_of(-1), {"shard": at(0, 1)}, plane_of(2)),),
    )

    def norm_start(step):
        for sem, sent, peer, _ in norm_steps[step]:
            norm_copy(sem, sent, peer).start()

    def norm_wait(step):
        for sem, sent, peer, arrived in norm_steps[step]:
            norm_copy(sem, sent, peer).wait_send()
            norm_copy(sem, arrived, peer).wait_recv()

    def launch(slot):
        for link in range(4):
            if (link, slot) == SHORT:
                pl.when(z == 3)(lambda: send(link, slot, cut_rows).start())
                pl.when(z != 3)(lambda: send(link, slot).start())
            else:
                send(link, slot).start()

    def receive(slot):
        for link in range(4):
            if (link, slot) == SHORT:
                pl.when(z == 0)(lambda: arrival(link, slot, SHIFT).wait_recv())
                pl.when(z != 0)(lambda: arrival(link, slot).wait_recv())
            else:
                arrival(link, slot).wait_recv()

    def sent(slots):
        for leaves, parts in (
            (0, out.at[pl.ds(0, slots), pl.ds(0, 3 * PART)]), (1, out.at[pl.ds(0, slots - 1), pl.ds(0, PART)])
        ):
            pltpu.make_async_copy(parts, parts, send_sem.at[leaves]).wait()
        pl.when(z == 3)(lambda: send(*SHORT, cut_rows).wait_send())
        pl.when(z != 3)(lambda: send(*SHORT).wait_send())
        pl.when(z == 1)(lambda: shifted(1).wait_send())

    norm_start(0)
    for step in range(3):
        norm_wait(step)
        norm_start(step + 1)
    for slot in range(2, AHEAD):
        launch(slot)
    first, last = min(BREAK), max(BREAK)
    breaks_late = core == BREAK.index(last)
    for slot in range(first):
        receive(slot)
        if slot in NORM_AT:
            norm_wait(NORM_AT[slot])
            if NORM_AT[slot] + 1 < len(norm_steps):
                norm_start(NORM_AT[slot] + 1)
        if slot == 1:
            pl.when(z == 1)(lambda: shifted(1).start())
        if slot == 6:
            pl.when(z == 0)(lambda: shifted(2).wait_recv())
        if slot + AHEAD < first:
            launch(slot + AHEAD)
        elif slot + AHEAD < last:
            pl.when(breaks_late)(lambda: launch(slot + AHEAD))
        if slot == max(NORM_AT):
            for row in range(64):
                even = norm_all[row // 4, (row % 4) * 2]
                odd = norm_all[row // 4, (row % 4) * 2 + 1]
                norm_rows[row:row + 1, :] = even + odd
            norm_out[...] = norm_rows[...].astype(jnp.bfloat16)

    @pl.when(breaks_late)
    def _():
        for slot in range(first, last):
            receive(slot)
            if slot + AHEAD < last:
                launch(slot + AHEAD)
        sent(last)

    @pl.when(jnp.logical_not(breaks_late))
    def _():
        sent(first)


def rest_kernel(block, norm, rest, send_sem, recv_sem, ready):
    shard, core, at = position()
    z, y = shard // 4, shard % 4
    later = (y < 3, y == 0, z < 3, z == 0)
    barrier = pltpu.get_barrier_semaphore()
    earlier_ones = 4
    for link, ((dy, dz), _) in enumerate(LINKS):
        earlier_ones = earlier_ones - later[link].astype(jnp.int32)

        @pl.when(later[link])
        def _():
            pl.semaphore_signal(barrier, inc=1, device_id={"shard": at(dy, dz)}, device_id_type=MESH)

    pl.when(earlier_ones > 0)(lambda: pl.semaphore_wait(barrier, earlier_ones))
    for link, ((dy, dz), _) in enumerate(LINKS):

        @pl.when(jnp.logical_not(later[link]))
        def _():
            pl.semaphore_signal(ready.at[link ^ 1], inc=1, device_id={"shard": at(dy, dz)}, device_id_type=MESH)

    def run(first):
        def copy(link, slot):
            (ty, tz), items = LINKS[link]
            dy, dz, part = items[slot]
            from_link, from_slot = PLACE.get(((dy + 1) % 4 - 1, (dz + 1) % 4 - 1, part), (0, -1))
            if from_slot < first:
                piece = block.at[at(dy, dz), pl.ds(part * PART, PART)]
            else:
                piece = rest.at[from_link, from_slot - first]
            return pltpu.make_async_remote_copy(
                src_ref=piece, dst_ref=rest.at[link, slot - first],
                send_sem=send_sem, recv_sem=recv_sem.at[link, slot - first],
                device_id={"shard": at(ty, tz)}, device_id_type=MESH,
            )

        def launch(link):
            for slot in range(first, SLOTS):
                copy(link, slot).start()

        for link in range(4):
            pl.when(jnp.logical_not(later[link]))(lambda: launch(link))
        for link in (0, 2, 1, 3):

            @pl.when(later[link])
            def _():
                pl.semaphore_wait(ready.at[link], 1)
                launch(link)

        for slot in range(first, SLOTS):
            for link in range(4):
                copy(link, slot).wait_recv()
        sent = rest.at[:, pl.ds(0, SLOTS - first)]
        pltpu.make_async_copy(sent, sent, send_sem).wait()

    for which in range(2):
        pl.when(core == which)(lambda: run(BREAK[which]))


def write_part(sem, src, owner, part, q, k, v):
    columns = pl.ds(pl.multiple_of(owner * COLS, COLS), COLS)
    row, count = part * PART, min(PART, 1024 - part * PART)
    pieces = [(0, count, q.at[pl.ds(row, count), columns])]
    if part == D:
        pieces += [(64, 128, k.at[:, columns]), (192, 128, v.at[:, columns])]
    for start, rows, dst in pieces:
        pltpu.make_async_copy(src.at[pl.ds(start, rows)], dst, sem).start()


def write_kernel(block, norm, q, k, v, n, sem, norm_sem):
    _, core, at = position()
    norm_copy = pltpu.make_async_copy(norm, n, norm_sem)
    norm_copy.start()

    def run(first):
        for part in range(4):
            for far in range(16):
                dy, dz = far % 4 - 1, far // 4 - 1
                if PLACE.get((dy, dz, part), (0, -1))[1] < first:
                    src = block.at[at(dy, dz), pl.ds(part * PART, PART)]
                    write_part(sem, src, at(dy, dz), part, q, k, v)
        blocks = block.at[pl.ds(0, 1 + first)]
        pltpu.make_async_copy(blocks, blocks, sem).wait()

    for which in range(2):
        pl.when(core == which)(lambda: run(BREAK[which]))
    norm_copy.wait()


def write_rest_kernel(rest, q_in, k_in, v_in, q, k, v, sem):
    _, core, at = position()

    def run(first):
        for (dy, dz, part), (link, slot) in PLACE.items():
            if slot >= first:
                write_part(sem, rest.at[link, slot - first], at(dy, dz), part, q, k, v)
        parts = rest.at[:, pl.ds(0, SLOTS - first)]
        pltpu.make_async_copy(parts, parts, sem).wait()

    for which in range(2):
        pl.when(core == which)(lambda: run(BREAK[which]))


def per_device(tq, lq, hq, tk, lk, hk, tv, lv, hv, nt, ns):
    hbm = pl.BlockSpec(memory_space=pltpu.HBM)
    vmem = pl.BlockSpec(memory_space=pltpu.VMEM)
    bf16, f32 = jnp.bfloat16, jnp.float32
    block, norm = pl.pallas_call(
        gather_kernel,
        out_shape=(pltpu.VMEM((16, ROWS, COLS), bf16), pltpu.VMEM((64, 128), bf16)),
        in_specs=[hbm] * 11,
        out_specs=(vmem, vmem),
        scratch_shapes=[
            pltpu.VMEM((10, COLS, TILE), bf16),
            pltpu.VMEM((3, 16, COLS), bf16),
            pltpu.VMEM((16, ROWS), bf16),
            pltpu.VMEM((1, 64), f32),
            pltpu.VMEM((1, 64), f32),
            pltpu.VMEM((16, 8, 1, 128), f32),
            pltpu.VMEM((64, 128), f32),
            pltpu.SemaphoreType.DMA((18,)),
            pltpu.SemaphoreType.DMA((3,)),
            pltpu.SemaphoreType.DMA((4, SLOTS)),
            pltpu.SemaphoreType.DMA((10,)),
            pltpu.SemaphoreType.DMA((10,)),
            pltpu.SemaphoreType.REGULAR((7,)),
            pltpu.SemaphoreType.DMA((2,)),
        ],
        compiler_params=pltpu.CompilerParams(
            collective_id=0, has_side_effects=True, vmem_limit_bytes=12 * 1024 * 1024
        ),
        name="gather",
    )(*(
        pltpu.with_memory_space_constraint(a, pltpu.HBM)
        for a in (tq, lq.T, hq, tk, lk.T, hk, tv, lv.T, hv, nt.reshape(1, 64), ns.reshape(1, 64))
    ))
    results = (
        jax.ShapeDtypeStruct((1024, 8192), bf16),
        jax.ShapeDtypeStruct((128, 8192), bf16),
        jax.ShapeDtypeStruct((128, 8192), bf16),
    )
    q, k, v, n = pl.pallas_call(
        write_kernel,
        out_shape=results + (jax.ShapeDtypeStruct((64, 128), bf16),),
        in_specs=[vmem, vmem],
        out_specs=(hbm,) * 4,
        scratch_shapes=[pltpu.SemaphoreType.DMA, pltpu.SemaphoreType.DMA],
        compiler_params=pltpu.CompilerParams(vmem_limit_bytes=4 * 1024 * 1024),
        name="write",
    )(block, norm)
    rest = pl.pallas_call(
        rest_kernel,
        out_shape=pltpu.VMEM((4, LATE, PART, COLS), bf16),
        in_specs=[vmem, hbm],
        out_specs=vmem,
        scratch_shapes=[
            pltpu.SemaphoreType.DMA, pltpu.SemaphoreType.DMA((4, LATE)), pltpu.SemaphoreType.REGULAR((4,))
        ],
        compiler_params=pltpu.CompilerParams(
            collective_id=1, has_side_effects=True, vmem_limit_bytes=4 * 1024 * 1024
        ),
        name="rest",
    )(block, pltpu.with_memory_space_constraint(n, pltpu.HBM))
    q, k, v = pl.pallas_call(
        write_rest_kernel,
        out_shape=results,
        in_specs=[vmem] + [hbm] * 3,
        out_specs=(hbm,) * 3,
        input_output_aliases={1: 0, 2: 1, 3: 2},
        scratch_shapes=[pltpu.SemaphoreType.DMA],
        compiler_params=pltpu.CompilerParams(vmem_limit_bytes=4 * 1024 * 1024),
        name="write_rest",
    )(rest, *(pltpu.with_memory_space_constraint(a, pltpu.HBM) for a in (q, k, v)))
    return q, k, v, n.reshape(8192)


def solution(mesh):
    in_specs = (
        P("shard", "tp"), P("shard", None), P(None, "tp"),
        P("shard", "tp"), P("shard", None), P(None, "tp"),
        P("shard", "tp"), P("shard", None), P(None, "tp"),
        P(("shard", "tp")), P(("shard", "tp")),
    )
    out_specs = (P("tp", None), P("tp", None), P("tp", None), P())
    return jax.shard_map(per_device, mesh=mesh, in_specs=in_specs, out_specs=out_specs, check_vma=False)
```

```python
import jax
import jax.numpy as jnp
from jax import lax
from jax.experimental import pallas as pl
from jax.experimental.pallas import tpu as pltpu
from jax.sharding import PartitionSpec as P

MESH = pl.DeviceIdType.MESH
mix_rate = 0.5

ROWS, COLS, TILE = 1280, 512, 128
PART = ROWS // 4
SLOTS = 15
A, B, C, D = 0, 1, 2, 3


def schedule():
    def order(first, second, own_first, own_second, step, place):
        side = lambda far: place(0, far)
        return [
            side(0) + (first,), side(0) + (second,), side(0) + (own_first,), side(0) + (own_second,),
            place(-step, 0) + (first,),
            side(-1) + (own_first,), side(-1) + (own_second,),
            place(-step, 0) + (own_first,),
            side(1) + (own_first,), side(1) + (own_second,),
            side(2) + (own_first,), side(2) + (own_second,),
            place(-step, -1) + (own_first,), place(-step, 1) + (own_first,), place(-step, 2) + (own_first,),
        ]

    along_y = lambda along, across: (along, across)
    along_z = lambda along, across: (across, along)
    return (
        ((1, 0), order(A, B, C, D, 1, along_y)),
        ((-1, 0), order(B, A, D, C, -1, along_y)),
        ((0, 1), order(C, D, A, B, 1, along_z)),
        ((0, -1), order(D, C, B, A, -1, along_z)),
    )


AHEAD = 4
NORM_AT = {1: 3, 4: 4, 7: 5, 10: 6}
BREAK = (14, 11)
LATE = SLOTS - min(BREAK)
LINKS = schedule()
SHORT, SHIFT = (2, 4), 48
ARRIVALS = [
    [(((dy - ty + 1) % 4) - 1, ((dz - tz + 1) % 4) - 1, part) for dy, dz, part in items] for (ty, tz), items in LINKS
]
PLACE = {ARRIVALS[link][slot]: (link, slot) for link in range(4) for slot in range(SLOTS)}
TILES = (
    (0, ((0, 0, 0, 128), (1, 1, 0, 128))),
    (5, ((2, 0, 640, 128), (3, 1, 640, 128))),
    (4, ((1, 0, 512, 128),)),
    (9, ((3, 0, 1152, 128),)),
    (1, ((0, 0, 128, 128),)),
    (6, ((2, 0, 768, 128),)),
    (3, ((1, 0, 384, 128),)),
    (8, ((3, 0, 1024, 128),)),
    (2, ((0, 0, 256, 64), (1, 0, 320, 64), (1, 1, 128, 192))),
    (7, ((2, 0, 896, 64), (3, 0, 960, 64), (3, 1, 768, 192))),
)


def position():
    shard, core = lax.axis_index("shard"), lax.axis_index("tp") % 2
    z, y = shard // 4, shard % 4

    def at(dy, dz):
        return ((z + dz + 4) % 4) * 4 + (y + dy + 4) % 4

    return shard, core, at


def gather_kernel(
    tq, lq, hq, tk, lk, hk, tv, lv, hv, nt, ns,
    out, norm_out,
    t_in, l_in, h_in, nt_in, ns_in, norm_all, norm_rows,
    load_sem, send_sem, recv_sem, norm_send, norm_recv, ready, shift_sem,
):
    shard, core, at = position()
    tp = lax.axis_index("tp")
    z, x = shard // 4, tp // 2

    def other(dx):
        return ((x + dx + 4) % 4) * 2 + core

    loads = {}

    def load(name, src, dst):
        loads[name] = pltpu.make_async_copy(src, dst, load_sem.at[len(loads)])
        loads[name].start()

    def load_tile(tile):
        if tile < 8:
            load(("t", tile), tq.at[:, pl.ds(tile * TILE, TILE)], t_in.at[tile])
        else:
            load(("t", tile), (tk, tv)[tile - 8], t_in.at[tile])

    for tile, _ in TILES[:2]:
        load_tile(tile)
    load(("l", 0), lq, l_in.at[0])
    load(("h", 0), hq, h_in.at[:, pl.ds(0, 1024)])
    load("nt", nt, nt_in)
    load("ns", ns, ns_in)

    y = shard % 4
    peers = [{"shard": at(dy, dz)} for (dy, dz), _ in LINKS]
    peers += [{"tp": x * 2 + 1 - core}, {"tp": other(1)}, {"tp": other(-1)}]
    mirror = (1, 0, 3, 2, 4, 6, 5)
    later = (y < 3, y == 0, z < 3, z == 0, core == 1, x < 3, x == 0)
    barrier = pltpu.get_barrier_semaphore()
    earlier_ones = 7
    for who, peer in enumerate(peers):
        earlier_ones = earlier_ones - later[who].astype(jnp.int32)

        @pl.when(later[who])
        def _():
            pl.semaphore_signal(barrier, inc=1, device_id=peer, device_id_type=MESH)

    for tile, _ in TILES[2:4]:
        load_tile(tile)
    load(("l", 2), lv, l_in.at[2])
    load(("h", 2), hv, h_in.at[:, pl.ds(1152, TILE)])
    load(("l", 1), lk, l_in.at[1])
    load(("h", 1), hk, h_in.at[:, pl.ds(1024, TILE)])
    for tile, _ in TILES[4:]:
        load_tile(tile)

    pl.when(earlier_ones > 0)(lambda: pl.semaphore_wait(barrier, earlier_ones))
    for who, peer in enumerate(peers):

        @pl.when(jnp.logical_not(later[who]))
        def _():
            pl.semaphore_signal(ready.at[mirror[who]], inc=1, device_id=peer, device_id_type=MESH)

    def greet(who):
        @pl.when(later[who])
        def _():
            pl.semaphore_wait(ready.at[who], 1)

    def copy(link, slot, owner, rows):
        piece = out.at[owner, pl.ds(*rows)]
        (dy, dz), _ = LINKS[link]
        leaves = send_sem.at[2 if (link, slot) == SHORT else (0, 0, 1, 0)[link]]
        return pltpu.make_async_remote_copy(
            src_ref=piece, dst_ref=piece, send_sem=leaves, recv_sem=recv_sem.at[link, slot],
            device_id={"shard": at(dy, dz)}, device_id_type=MESH,
        )

    def send(link, slot, rows=None):
        dy, dz, part = LINKS[link][1][slot]
        return copy(link, slot, at(dy, dz), rows if rows is not None else (part * PART, PART))

    def arrival(link, slot, cut=0):
        (ty, tz), items = LINKS[link]
        dy, dz, part = items[slot]
        return copy(link, slot, at(dy - ty, dz - tz), (part * PART, PART - cut))

    part = LINKS[SHORT[0]][1][SHORT[1]][2]
    cut_rows, shifted_rows = (part * PART, PART - SHIFT), (part * PART + PART - SHIFT, SHIFT)

    def shifted(dz):
        piece = out.at[at(0, dz), pl.ds(*shifted_rows)]
        return pltpu.make_async_remote_copy(
            src_ref=piece, dst_ref=piece, send_sem=shift_sem.at[0], recv_sem=shift_sem.at[1],
            device_id={"shard": at(0, -1)}, device_id_type=MESH,
        )

    def merge(tile):
        loads[("t", tile)].wait()
        which = max(tile - 7, 0)
        for name in (("l", which), ("h", which)):
            if name in loads:
                loads.pop(name).wait()
        product = lax.dot_general(
            h_in[:, tile * TILE:(tile + 1) * TILE], l_in[which], (((0,), (0,)), ((), ())),
            preferred_element_type=jnp.float32,
        )
        whole = t_in[tile].astype(jnp.float32).T + mix_rate * product
        out[shard, tile * TILE:(tile + 1) * TILE, :] = whole.astype(jnp.bfloat16)

    def send_pieces(pieces):
        for link, slot, row, count in pieces:
            pl.when(jnp.logical_not(later[link]))(lambda: send(link, slot, (row, count)).start())

    waiting = ()
    for tile, pieces in TILES:
        merge(tile)
        send_pieces(waiting)
        waiting = pieces

    loads["nt"].wait()
    loads["ns"].wait()
    gain = nt_in[...] + ns_in[...]
    both = jnp.concatenate([gain, gain], axis=1)
    half = lax.broadcasted_iota(jnp.int32, (1, 128), 1) // 64
    norm_all[shard, tp] = jnp.where(half == core, both, 0.0)

    send_pieces(waiting)
    for link in (0, 2):
        pl.when(jnp.logical_not(later[link]))(lambda: send(link, 1).start())
    for link in (0, 2, 1, 3):

        @pl.when(later[link])
        def _():
            pl.semaphore_wait(ready.at[link], 1)
            send(link, 0).start()
            send(link, 1).start()

    for who in (4, 5, 6):
        greet(who)

    def norm_copy(step, piece, peer):
        return pltpu.make_async_remote_copy(
            src_ref=piece, dst_ref=piece, send_sem=norm_send.at[step], recv_sem=norm_recv.at[step],
            device_id=peer, device_id_type=MESH,
        )

    def pair(dx):
        return norm_all.at[shard, pl.ds(((x + dx + 4) % 4) * 2, 2)]

    def row_of(dy):
        return norm_all.at[at(dy, 0)]

    def plane_of(dz):
        return norm_all.at[pl.ds(((z + dz + 4) % 4) * 4, 4)]

    own = norm_all.at[shard, tp]
    twin = norm_all.at[shard, x * 2 + 1 - core]
    norm_steps = (
        ((0, own, {"tp": x * 2 + 1 - core}, twin),),
        ((1, pair(0), {"tp": other(1)}, pair(-1)), (2, pair(0), {"tp": other(-1)}, pair(1))),
        ((3, pair(-1), {"tp": other(1)}, pair(2)),),
        ((4, row_of(0), {"shard": at(1, 0)}, row_of(-1)), (5, row_of(0), {"shard": at(-1, 0)}, row_of(1))),
        ((6, row_of(-1), {"shard": at(1, 0)}, row_of(2)),),
        ((7, plane_of(0), {"shard": at(0, 1)}, plane_of(-1)), (8, plane_of(0), {"shard": at(0, -1)}, plane_of(1))),
        ((9, plane_of(-1), {"shard": at(0, 1)}, plane_of(2)),),
    )

    def norm_start(step):
        for sem, sent, peer, _ in norm_steps[step]:
            norm_copy(sem, sent, peer).start()

    def norm_wait(step):
        for sem, sent, peer, arrived in norm_steps[step]:
            norm_copy(sem, sent, peer).wait_send()
            norm_copy(sem, arrived, peer).wait_recv()

    def launch(slot):
        for link in range(4):
            if (link, slot) == SHORT:
                pl.when(z == 3)(lambda: send(link, slot, cut_rows).start())
                pl.when(z != 3)(lambda: send(link, slot).start())
            else:
                send(link, slot).start()

    def receive(slot):
        for link in range(4):
            if (link, slot) == SHORT:
                pl.when(z == 0)(lambda: arrival(link, slot, SHIFT).wait_recv())
                pl.when(z != 0)(lambda: arrival(link, slot).wait_recv())
            else:
                arrival(link, slot).wait_recv()

    def sent(slots):
        for leaves, parts in (
            (0, out.at[pl.ds(0, slots), pl.ds(0, 3 * PART)]), (1, out.at[pl.ds(0, slots - 1), pl.ds(0, PART)])
        ):
            pltpu.make_async_copy(parts, parts, send_sem.at[leaves]).wait()
        pl.when(z == 3)(lambda: send(*SHORT, cut_rows).wait_send())
        pl.when(z != 3)(lambda: send(*SHORT).wait_send())
        pl.when(z == 1)(lambda: shifted(1).wait_send())

    norm_start(0)
    for step in range(3):
        norm_wait(step)
        norm_start(step + 1)
    for slot in range(2, AHEAD):
        launch(slot)
    first, last = min(BREAK), max(BREAK)
    breaks_late = core == BREAK.index(last)
    for slot in range(first):
        receive(slot)
        if slot in NORM_AT:
            norm_wait(NORM_AT[slot])
            if NORM_AT[slot] + 1 < len(norm_steps):
                norm_start(NORM_AT[slot] + 1)
        if slot == 1:
            pl.when(z == 1)(lambda: shifted(1).start())
        if slot == 6:
            pl.when(z == 0)(lambda: shifted(2).wait_recv())
        if slot + AHEAD < first:
            launch(slot + AHEAD)
        elif slot + AHEAD < last:
            pl.when(breaks_late)(lambda: launch(slot + AHEAD))
        if slot == max(NORM_AT):
            for row in range(64):
                even = norm_all[row // 4, (row % 4) * 2]
                odd = norm_all[row // 4, (row % 4) * 2 + 1]
                norm_rows[row:row + 1, :] = even + odd
            norm_out[...] = norm_rows[...].astype(jnp.bfloat16)

    @pl.when(breaks_late)
    def _():
        for slot in range(first, last):
            receive(slot)
            if slot + AHEAD < last:
                launch(slot + AHEAD)
        sent(last)

    @pl.when(jnp.logical_not(breaks_late))
    def _():
        sent(first)


def rest_kernel(block, norm, rest, send_sem, recv_sem, ready):
    shard, core, at = position()
    z, y = shard // 4, shard % 4
    later = (y < 3, y == 0, z < 3, z == 0)
    barrier = pltpu.get_barrier_semaphore()
    earlier_ones = 4
    for link, ((dy, dz), _) in enumerate(LINKS):
        earlier_ones = earlier_ones - later[link].astype(jnp.int32)

        @pl.when(later[link])
        def _():
            pl.semaphore_signal(barrier, inc=1, device_id={"shard": at(dy, dz)}, device_id_type=MESH)

    pl.when(earlier_ones > 0)(lambda: pl.semaphore_wait(barrier, earlier_ones))
    for link, ((dy, dz), _) in enumerate(LINKS):

        @pl.when(jnp.logical_not(later[link]))
        def _():
            pl.semaphore_signal(ready.at[link ^ 1], inc=1, device_id={"shard": at(dy, dz)}, device_id_type=MESH)

    def run(first):
        def copy(link, slot):
            (ty, tz), items = LINKS[link]
            dy, dz, part = items[slot]
            from_link, from_slot = PLACE.get(((dy + 1) % 4 - 1, (dz + 1) % 4 - 1, part), (0, -1))
            if from_slot < first:
                piece = block.at[at(dy, dz), pl.ds(part * PART, PART)]
            else:
                piece = rest.at[from_link, from_slot - first]
            return pltpu.make_async_remote_copy(
                src_ref=piece, dst_ref=rest.at[link, slot - first],
                send_sem=send_sem, recv_sem=recv_sem.at[link, slot - first],
                device_id={"shard": at(ty, tz)}, device_id_type=MESH,
            )

        def launch(link):
            for slot in range(first, SLOTS):
                copy(link, slot).start()

        for link in range(4):
            pl.when(jnp.logical_not(later[link]))(lambda: launch(link))
        for link in (0, 2, 1, 3):

            @pl.when(later[link])
            def _():
                pl.semaphore_wait(ready.at[link], 1)
                launch(link)

        for slot in range(first, SLOTS):
            for link in range(4):
                copy(link, slot).wait_recv()
        sent = rest.at[:, pl.ds(0, SLOTS - first)]
        pltpu.make_async_copy(sent, sent, send_sem).wait()

    for which in range(2):
        pl.when(core == which)(lambda: run(BREAK[which]))


def write_part(sem, src, owner, part, q, k, v, cuts=1):
    columns = pl.ds(pl.multiple_of(owner * COLS, COLS), COLS)
    row, count = part * PART, min(PART, 1024 - part * PART)
    step = count // cuts
    pieces = [(at, step, q.at[pl.ds(row + at, step), columns]) for at in range(0, count, step)]
    if part == D:
        pieces += [(64, 128, k.at[:, columns]), (192, 128, v.at[:, columns])]
    for start, rows, dst in pieces:
        pltpu.make_async_copy(src.at[pl.ds(start, rows)], dst, sem).start()


def write_kernel(block, norm, q, k, v, n, sem, norm_sem):
    _, core, at = position()
    norm_copy = pltpu.make_async_copy(norm, n, norm_sem)
    norm_copy.start()

    def run(first):
        for part in range(4):
            for far in range(16):
                dy, dz = far % 4 - 1, far // 4 - 1
                if PLACE.get((dy, dz, part), (0, -1))[1] < first:
                    src = block.at[at(dy, dz), pl.ds(part * PART, PART)]
                    write_part(sem, src, at(dy, dz), part, q, k, v)
        blocks = block.at[pl.ds(0, 1 + first)]
        pltpu.make_async_copy(blocks, blocks, sem).wait()

    for which in range(2):
        pl.when(core == which)(lambda: run(BREAK[which]))
    norm_copy.wait()


def write_rest_kernel(rest, q_in, k_in, v_in, q, k, v, sem):
    _, core, at = position()

    def run(first):
        for (dy, dz, part), (link, slot) in PLACE.items():
            if slot >= first:
                write_part(sem, rest.at[link, slot - first], at(dy, dz), part, q, k, v, 4 if slot >= max(BREAK) else 1)
        parts = rest.at[:, pl.ds(0, SLOTS - first)]
        pltpu.make_async_copy(parts, parts, sem).wait()

    for which in range(2):
        pl.when(core == which)(lambda: run(BREAK[which]))


def per_device(tq, lq, hq, tk, lk, hk, tv, lv, hv, nt, ns):
    hbm = pl.BlockSpec(memory_space=pltpu.HBM)
    vmem = pl.BlockSpec(memory_space=pltpu.VMEM)
    bf16, f32 = jnp.bfloat16, jnp.float32
    block, norm = pl.pallas_call(
        gather_kernel,
        out_shape=(pltpu.VMEM((16, ROWS, COLS), bf16), pltpu.VMEM((64, 128), bf16)),
        in_specs=[hbm] * 11,
        out_specs=(vmem, vmem),
        scratch_shapes=[
            pltpu.VMEM((10, COLS, TILE), bf16),
            pltpu.VMEM((3, 16, COLS), bf16),
            pltpu.VMEM((16, ROWS), bf16),
            pltpu.VMEM((1, 64), f32),
            pltpu.VMEM((1, 64), f32),
            pltpu.VMEM((16, 8, 1, 128), f32),
            pltpu.VMEM((64, 128), f32),
            pltpu.SemaphoreType.DMA((18,)),
            pltpu.SemaphoreType.DMA((3,)),
            pltpu.SemaphoreType.DMA((4, SLOTS)),
            pltpu.SemaphoreType.DMA((10,)),
            pltpu.SemaphoreType.DMA((10,)),
            pltpu.SemaphoreType.REGULAR((7,)),
            pltpu.SemaphoreType.DMA((2,)),
        ],
        compiler_params=pltpu.CompilerParams(
            collective_id=0, has_side_effects=True, vmem_limit_bytes=12 * 1024 * 1024
        ),
        name="gather",
    )(*(
        pltpu.with_memory_space_constraint(a, pltpu.HBM)
        for a in (tq, lq.T, hq, tk, lk.T, hk, tv, lv.T, hv, nt.reshape(1, 64), ns.reshape(1, 64))
    ))
    results = (
        jax.ShapeDtypeStruct((1024, 8192), bf16),
        jax.ShapeDtypeStruct((128, 8192), bf16),
        jax.ShapeDtypeStruct((128, 8192), bf16),
    )
    q, k, v, n = pl.pallas_call(
        write_kernel,
        out_shape=results + (jax.ShapeDtypeStruct((64, 128), bf16),),
        in_specs=[vmem, vmem],
        out_specs=(hbm,) * 4,
        scratch_shapes=[pltpu.SemaphoreType.DMA, pltpu.SemaphoreType.DMA],
        compiler_params=pltpu.CompilerParams(vmem_limit_bytes=4 * 1024 * 1024),
        name="write",
    )(block, norm)
    rest = pl.pallas_call(
        rest_kernel,
        out_shape=pltpu.VMEM((4, LATE, PART, COLS), bf16),
        in_specs=[vmem, hbm],
        out_specs=vmem,
        scratch_shapes=[
            pltpu.SemaphoreType.DMA, pltpu.SemaphoreType.DMA((4, LATE)), pltpu.SemaphoreType.REGULAR((4,))
        ],
        compiler_params=pltpu.CompilerParams(
            collective_id=1, has_side_effects=True, vmem_limit_bytes=4 * 1024 * 1024
        ),
        name="rest",
    )(block, pltpu.with_memory_space_constraint(n, pltpu.HBM))
    q, k, v = pl.pallas_call(
        write_rest_kernel,
        out_shape=results,
        in_specs=[vmem] + [hbm] * 3,
        out_specs=(hbm,) * 3,
        input_output_aliases={1: 0, 2: 1, 3: 2},
        scratch_shapes=[pltpu.SemaphoreType.DMA],
        compiler_params=pltpu.CompilerParams(vmem_limit_bytes=4 * 1024 * 1024),
        name="write_rest",
    )(rest, *(pltpu.with_memory_space_constraint(a, pltpu.HBM) for a in (q, k, v)))
    return q, k, v, n.reshape(8192)


def solution(mesh):
    in_specs = (
        P("shard", "tp"), P("shard", None), P(None, "tp"),
        P("shard", "tp"), P("shard", None), P(None, "tp"),
        P("shard", "tp"), P("shard", None), P(None, "tp"),
        P(("shard", "tp")), P(("shard", "tp")),
    )
    out_specs = (P("tp", None), P("tp", None), P("tp", None), P())
    return jax.shard_map(per_device, mesh=mesh, in_specs=in_specs, out_specs=out_specs, check_vma=False)
```
